32 devices in a mesh: seq: 16 (over z, x, core), head: 2 (over y).
Axes of the slice: x: 2, y: 2, z: 4, core: 2. Of those that a mesh axis runs over, the one named last changes fastest.
Arguments:
- query: bfloat16 [1, 4096, 2048], P(None, 'seq', 'head'), may hold values from -210 to 210
- keys: bfloat16 [1, 4096, 512], P(None, 'seq', 'head'), may hold values from -7 to 7
- values: bfloat16 [1, 4096, 512], P(None, 'seq', 'head'), may hold values from -6 to 6
- grad_out: bfloat16 [1, 4096, 2048], P(None, 'seq', 'head'), may hold values from -6 to 6
- global_offset: int32 [1, 64], replicated, may hold values from 0 to 255, as said below
- owner: int32 [16], replicated, may hold values from 0 to 15, each once
- block_lists: int32 [1, 32, 3], P(None, 'seq'), may hold values from 0 to 31, as said below
Outputs:
- grad_query: bfloat16 [1, 4096, 2048], P(None, 'seq', 'head')
- grad_keys: bfloat16 [1, 4096, 512], P(None, 'seq', 'head')
- grad_values: bfloat16 [1, 4096, 512], P(None, 'seq', 'head')
The draws below stay inside these ranges and needn't reach their ends.
Inputs may be any that keep to these rules, and one draw needn't show every extreme that they name: `block_lists`: row b of each layer lists b first, then 3 - 1 other distinct blocks within 2 blocks of b. `global_offset`: distinct within a layer. `owner`: each sequence shard appears once.
All inputs are finite; a program needn't handle non-finite values.
Results may differ from the reference program's by a relative error of at most 0.02.
Values may be sent and summed in bfloat16 or wider, within the bound.
A program may use at most 64 MiB of HBM per device.

```python
import jax
import jax.numpy as jnp
from jax import lax

HQ = 16
HK = 4
DH = 128
LAYERS = 1
BLOCK = 128
REACH = 2
LISTED = 3
G = 64
TOK_DEV = 256
SEQ = 4096
NBLK = 32
N_SEQ = 16


def shared_draw(key):
    full_shape = (LAYERS, SEQ, HK * DH)
    base_keys = jax.random.truncated_normal(jax.random.fold_in(key, 101), -6.0, 6.0, full_shape, jnp.float32)
    return base_keys


def draw_keys(key, part):
    base_keys = shared_draw(key)
    return base_keys.astype(jnp.bfloat16)


def draw_query(key, part):
    drawn = jax.random.truncated_normal(jax.random.fold_in(key, 201), -6.0, 6.0, (LAYERS, SEQ, HQ * DH), jnp.float32)
    return drawn.astype(jnp.bfloat16)


def draw_global_offset(key, part):
    ranks = jax.random.randint(jax.random.fold_in(key, 301), (LAYERS, TOK_DEV), 0, 65536) * TOK_DEV + jnp.arange(TOK_DEV)
    unused, picked = lax.top_k(ranks, G)
    return picked.astype(jnp.int32)


def draw_block_lists(key, part):
    offsets = jnp.concatenate([jnp.arange(-REACH, 0), jnp.arange(1, REACH + 1)])
    block_ids = jnp.arange(NBLK)
    candidate = block_ids[:, None] + offsets[None, :]
    inside = (candidate >= 0) & (candidate < NBLK)
    ranks = jax.random.randint(jax.random.fold_in(key, 401), (LAYERS, NBLK, 2 * REACH), 0, 65536) * (2 * REACH) + jnp.arange(2 * REACH)
    ranks = jnp.where(inside[None], ranks, -1 - jnp.arange(2 * REACH))
    unused, picked = lax.top_k(ranks, LISTED - 1)
    others = jnp.take_along_axis(jnp.broadcast_to(candidate, (LAYERS, NBLK, 2 * REACH)), picked, axis=2)
    itself = jnp.broadcast_to(block_ids[None, :, None], (LAYERS, NBLK, 1))
    return jnp.concatenate([itself, others], axis=2).astype(jnp.int32)


def block_scale(rng, extent, pieces, low, top_value):
    loudness = 1.0
    for dim, blocks in pieces:
        steps = jax.random.uniform(jax.random.fold_in(jax.random.fold_in(rng, 6), dim), (blocks,), jnp.float32, low / len(pieces), top_value / len(pieces))
        loudness = loudness * jnp.repeat(jnp.exp(steps), extent[dim] // blocks).reshape((-1,) + (1,) * (len(extent) - 1 - dim))
    return loudness


def gaussian(stream_key, extent, spread, bound, cuts=(), dtype=jnp.bfloat16):
    drawn = spread * jax.random.normal(stream_key, extent, jnp.float32)
    if cuts:
        drawn = drawn * block_scale(stream_key, extent, cuts, -0.22, 0.18)
    return jnp.clip(drawn, -bound, bound).astype(dtype)


def setup_inputs(seed: int = 0) -> dict:
    arg_keys = jax.random.split(jax.random.key(seed), 8)
    query = draw_query(jax.random.fold_in(arg_keys[7], 71), 0)
    keys = draw_keys(jax.random.fold_in(arg_keys[7], 71), 0)
    values = gaussian(arg_keys[2], (LAYERS, SEQ, HK * DH), 1.0, 6.0, ((1, 16), (2, 2)))
    grad_out = gaussian(arg_keys[3], (LAYERS, SEQ, HQ * DH), 1.0, 6.0, ((1, 16), (2, 2)))
    global_offset = draw_global_offset(jax.random.fold_in(arg_keys[7], 71), 0)
    owner = jax.random.permutation(arg_keys[5], N_SEQ).astype(jnp.int32)
    block_lists = draw_block_lists(jax.random.fold_in(arg_keys[7], 71), 0)
    return {"query": query, "keys": keys, "values": values, "grad_out": grad_out, "global_offset": global_offset, "owner": owner, "block_lists": block_lists}


def scores(q_block, k_rows):
    return jnp.einsum("tcgd,scd->cgts", q_block.astype(jnp.float32), k_rows.astype(jnp.float32)) * (DH ** -0.5)


def backward(q_block, g_block, k_rows, v_rows, attn_probs, out_dot):
    attn_half = lax.optimization_barrier(attn_probs.astype(jnp.bfloat16))
    grad_probs = jnp.einsum("tcgd,scd->cgts", g_block.astype(jnp.float32), v_rows.astype(jnp.float32))
    grad_logits = lax.optimization_barrier((attn_probs * (grad_probs - out_dot[..., None])).astype(jnp.bfloat16))
    grad_q = jnp.einsum("cgts,scd->tcgd", grad_logits.astype(jnp.float32), k_rows.astype(jnp.float32)) * (DH ** -0.5)
    grad_k = jnp.einsum("cgts,tcgd->scd", grad_logits.astype(jnp.float32), q_block.astype(jnp.float32)) * (DH ** -0.5)
    grad_v = jnp.einsum("cgts,tcgd->scd", attn_half.astype(jnp.float32), g_block.astype(jnp.float32))
    return grad_q, grad_k, grad_v


def attend(q_block, g_block, k_rows, v_rows):
    logits = scores(q_block, k_rows)
    top_logit = jnp.max(logits, axis=-1, keepdims=True)
    log_total = top_logit + jnp.log(jnp.sum(jnp.exp(logits - top_logit), axis=-1, keepdims=True))
    attn_probs = jnp.exp(logits - log_total)
    attn_half = lax.optimization_barrier(attn_probs.astype(jnp.bfloat16))
    output = jnp.einsum("cgts,scd->tcgd", attn_half.astype(jnp.float32), v_rows.astype(jnp.float32)).astype(jnp.bfloat16)
    output = lax.optimization_barrier(output)
    out_dot = jnp.einsum("tcgd,tcgd->cgt", g_block.astype(jnp.float32), output.astype(jnp.float32))
    return backward(q_block, g_block, k_rows, v_rows, attn_probs, out_dot)


def reference(query, keys, values, grad_out, global_offset, owner, block_lists):
    group_size = HQ // HK
    window_len = LISTED * BLOCK
    kv_width = HK * DH
    grads_q = []
    grads_k = []
    grads_v = []
    for layer_idx in range(LAYERS):
        key_blocks = keys[layer_idx].reshape(NBLK, BLOCK, HK, DH)
        value_blocks = values[layer_idx].reshape(NBLK, BLOCK, HK, DH)
        global_pos = (owner[layer_idx] * TOK_DEV + global_offset[layer_idx]).astype(jnp.int32)
        global_k = keys[layer_idx][global_pos].reshape(G, HK, DH)
        global_v = values[layer_idx][global_pos].reshape(G, HK, DH)
        q_blocks = query[layer_idx].reshape(NBLK, BLOCK, HK, group_size, DH)
        g_blocks = grad_out[layer_idx].reshape(NBLK, BLOCK, HK, group_size, DH)

        def block_step(state_sums, inputs):
            sum_k, sum_v, glob_k, glob_v = state_sums
            q_block, g_block, block_idx = inputs
            block_idx = block_idx.astype(jnp.int32)
            k_rows = jnp.concatenate([key_blocks[block_idx].reshape(window_len, HK, DH), global_k], axis=0)
            v_rows = jnp.concatenate([value_blocks[block_idx].reshape(window_len, HK, DH), global_v], axis=0)
            grad_q, grad_k, grad_v = attend(q_block, g_block, k_rows, v_rows)
            sum_k = sum_k.at[block_idx].add(grad_k[:window_len].reshape(LISTED, BLOCK, kv_width))
            sum_v = sum_v.at[block_idx].add(grad_v[:window_len].reshape(LISTED, BLOCK, kv_width))
            glob_k = glob_k + grad_k[window_len:].reshape(G, kv_width)
            glob_v = glob_v + grad_v[window_len:].reshape(G, kv_width)
            return (sum_k, sum_v, glob_k, glob_v), grad_q.astype(jnp.bfloat16).reshape(BLOCK, HQ * DH)

        zero_state = (jnp.zeros((NBLK, BLOCK, kv_width), jnp.float32), jnp.zeros((NBLK, BLOCK, kv_width), jnp.float32),
                      jnp.zeros((G, kv_width), jnp.float32), jnp.zeros((G, kv_width), jnp.float32))
        final, grad_q_blocks = lax.scan(block_step, zero_state, (q_blocks, g_blocks, block_lists[layer_idx]))
        total_k = final[0].reshape(SEQ, kv_width).at[global_pos].add(final[2])
        total_v = final[1].reshape(SEQ, kv_width).at[global_pos].add(final[3])
        grads_q.append(grad_q_blocks.reshape(SEQ, HQ * DH))
        grads_k.append(total_k.astype(jnp.bfloat16))
        grads_v.append(total_v.astype(jnp.bfloat16))
    return jnp.stack(grads_q), jnp.stack(grads_k), jnp.stack(grads_v)
```

```python
import functools

import jax
import jax.numpy as jnp
from jax import lax
from jax.experimental import pallas as pl
from jax.experimental.pallas import tpu as pltpu
from jax.sharding import PartitionSpec as P

HQ = 16
HK = 4
DH = 128
BLOCK = 128
REACH = 2
LOG2E = 1.4426950408889634
F32 = jnp.float32
BF16 = jnp.bfloat16


def nt(a, b):
    return lax.dot_general(a, b, (((1,), (1,)), ((), ())), preferred_element_type=F32)


def nn(a, b):
    return lax.dot_general(a, b, (((1,), (0,)), ((), ())), preferred_element_type=F32)


def kernel(
    n, heads, group, nb, listed, gtok,
    owner_hbm, lists_hbm, goff_hbm, q_hbm, k_hbm, v_hbm, g_hbm,
    dq_ref, dk_ref, dv_ref,
    owner_ref, lists_ref, goff_ref, small_sem, qv, gv, gsend, hub_in, hub_out, gall, gpart, hub2_in, cross_out, cross_in, hub2_out, gall2, cross_sem,
    keep_ex, keep_dp, keep_ds, wslot, own, sback, rback, load_sem, big_sem, ks_sem, kr_sem, gs_sem, gr_sem, hs_sem, hr_sem,
    *kvw,
):
    me = lax.axis_index("seq")
    hubs = 2 * heads
    rows = nb * BLOCK
    first = n // 2 - hubs + 1
    hub = (me - first) // 2
    col = lax.rem(me // 2, 2)
    lane = (me // 4) * 2 + lax.rem(me, 2)
    level = hub // 2
    group_of = jnp.where(col == 0, level, heads - 1 - level)
    other_hub = first + 2 * (hubs - 1 - hub)

    def hub_id(g):
        return first + jnp.where(col == 0, 4 * g, 4 * (heads - 1 - g) + 2)

    def hubbed(i):
        return (i >= first) & (i < first + 2 * hubs) & (lax.rem(i + first, 2) == 0)

    barrier = pltpu.get_barrier_semaphore()

    def greet(other):
        pl.semaphore_signal(
            barrier, inc=1, device_id={"seq": other}, device_id_type=pl.DeviceIdType.MESH
        )

    mine_hub = hubbed(me)

    @pl.when(mine_hub)
    def _():
        @pl.loop(1, n)
        def _(i):
            greet(lax.rem(me + i, n))

    @pl.when(~mine_hub)
    def _():
        @pl.when(me > 0)
        def _():
            greet(me - 1)

        @pl.when(me < n - 1)
        def _():
            greet(me + 1)

    src_refs = (k_hbm, v_hbm)
    loads = []
    for t in range(2):
        for c in range(heads):
            for i in range(nb):
                cp = pltpu.make_async_copy(
                    src_refs[t].at[0, pl.ds(i * BLOCK, BLOCK), pl.ds(c * DH, DH)],
                    kvw[t * heads + c].at[REACH + i],
                    load_sem.at[(t * heads + c) * nb + i],
                )
                cp.start()
                loads.append(cp)
    small = [
        pltpu.make_async_copy(a, b, small_sem.at[i])
        for i, (a, b) in enumerate(
            ((goff_hbm, goff_ref), (owner_hbm, owner_ref), (lists_hbm, lists_ref))
        )
    ]
    for cp in small:
        cp.start()
    cq = pltpu.make_async_copy(q_hbm.at[0], qv, big_sem.at[0])
    cg = pltpu.make_async_copy(g_hbm.at[0], gv, big_sem.at[1])
    cq.start()
    cg.start()

    with jax.named_scope("w_loads"):
        small[0].wait()
        for cp in loads:
            cp.wait()

    hot = lax.broadcasted_iota(jnp.int32, (rows, gtok), 0) == goff_ref[...]
    hot = jnp.where(hot, 1.0, 0.0).astype(BF16)
    for t in range(2):
        for c in range(heads):
            mine = kvw[t * heads + c][REACH : REACH + nb].reshape(rows, DH)
            got = lax.dot_general(hot, mine, (((0,), (0,)), ((), ())), preferred_element_type=F32)
            gsend[t * heads + c] = got.astype(BF16)
    zeros_kv = jnp.zeros((REACH, BLOCK, DH), BF16)

    @pl.when(me == 0)
    def _():
        for ref in kvw:
            ref[0:REACH] = zeros_kv
        rback[0] = jnp.zeros(rback.shape[1:], BF16)

    @pl.when(me == n - 1)
    def _():
        for ref in kvw:
            ref[REACH + nb : REACH + nb + REACH] = zeros_kv
        rback[1] = jnp.zeros(rback.shape[1:], BF16)

    zero_tile = jnp.zeros((nb, 2, BLOCK, DH), F32)
    wslot[:, listed] = zero_tile

    below = jnp.where((me > 0) & ~hubbed(me - 1), 1, 0)
    above = jnp.where((me < n - 1) & ~hubbed(me + 1), 1, 0)
    with jax.named_scope("w_barrier"):
        pl.semaphore_wait(barrier, jnp.where(mine_hub, hubs - 1, hubs) + below + above)

    def remote(src, dst, s_sem, r_sem, target):
        return pltpu.make_async_remote_copy(
            src_ref=src, dst_ref=dst, send_sem=s_sem, recv_sem=r_sem,
            device_id={"seq": target}, device_id_type=pl.DeviceIdType.MESH,
        )

    def hub_send(src, dst, s_sem, r_sem, j):
        @pl.when(me != first + 2 * j)
        def _():
            remote(src.at[j], dst.at[me], s_sem, r_sem, first + 2 * j).start()

    def drain(ref, count, sem):
        part = ref.at[pl.ds(0, count)]
        pltpu.make_async_copy(part, part, sem).wait()

    def hub_sends(src, dst, i):
        for j in range(hubs):
            hub_send(src, dst, hs_sem.at[i], hr_sem.at[i], j)

    hub_sends(gsend, hub_in, 0)

    def halo(direction, c, t):
        idx = (direction * heads + c) * 2 + t
        ref = kvw[t * heads + c]
        if direction == 0:
            src, dst, target = ref.at[pl.ds(nb, REACH)], ref.at[pl.ds(0, REACH)], me + 1
        else:
            src, dst, target = ref.at[pl.ds(REACH, REACH)], ref.at[pl.ds(REACH + nb, REACH)], me - 1
        return remote(src, dst, ks_sem.at[idx], kr_sem.at[idx], target)

    def back(direction, c):
        idx = direction * heads + c
        target = me + 1 if direction == 0 else me - 1
        return remote(
            sback.at[direction, c], rback.at[direction, c], gs_sem.at[idx], gr_sem.at[idx], target
        )

    def each(direction, receiving, what):
        up = (direction == 0) != receiving
        cond = me < n - 1 if up else me > 0
        pl.when(cond)(what)

    place = lax.rem(me, 4)

    def far(d):
        return place == (3 if d == 0 else 0)

    def halo_start(c, d, late):
        for t in range(2):
            cond = (me < n - 1 if d == 0 else me > 0) & (far(d) if late else ~far(d))
            pl.when(cond)(lambda t=t: halo(d, c, t).start())

    held = mine_hub & (place == 1)

    halo_start(0, 0, False)
    halo_start(0, 1, False)
    for c in range(1, heads):
        halo_start(c, 1, False)
        pl.when(~held)(functools.partial(halo_start, c, 0, False))

    even = lax.rem(me, 2) == 0

    def halo_wait(c, paired):
        for d in range(2):
            cond = (me > 0 if d == 0 else me < n - 1) & ((even if d == 1 else ~even) == paired)
            for t in range(2):
                pl.when(cond)(lambda d=d, t=t: halo(d, c, t).wait_recv())

    with jax.named_scope("w_pair"):
        halo_wait(0, True)
    for c in range(heads):
        for d in range(2):
            halo_start(c, d, True)

    for cp in small[1:]:
        cp.wait()

    def broadcast(src, dst, i):
        @pl.loop(1, n)
        def _(k):
            remote(src, dst.at[hub], hs_sem.at[i], hr_sem.at[i], lax.rem(me + k, n)).start()

    @pl.when(mine_hub)
    def _():
        hub_in[me] = gsend[hub]
        with jax.named_scope("w_hub1"):
            drain(hub_in, n - 1, hr_sem.at[0])
        pick = hub_in[owner_ref[0]]
        hub_out[...] = pick
        gall[hub] = pick
        broadcast(hub_out, gall, 1)

        @pl.when(held)
        def _():
            for c in range(1, heads):
                halo_start(c, 0, False)

    with jax.named_scope('w_qg'):
        cq.wait()
        cg.wait()
    scale = DH ** (-0.5)
    fold = scale * LOG2E
    local_idx = [
        [
            jnp.clip(lists_ref[0, b, l] - me * nb + REACH, 0, nb + 2 * REACH - 1)
            for l in range(listed)
        ]
        for b in range(nb)
    ]

    def listed_rows(t, c, b):
        return jnp.concatenate([kvw[t * heads + c][local_idx[b][l]] for l in range(listed)], axis=0)

    def global_rows(ref, t, c):
        return ref[t * heads + c]

    def columns(c):
        return [slice((c * group + i) * DH, (c * group + i + 1) * DH) for i in range(group)]

    def stacked(ref, c, b):
        rsl = slice(b * BLOCK, (b + 1) * BLOCK)
        return jnp.concatenate([ref[rsl, s] for s in columns(c)], axis=0)

    def back_start(c):
        for d in range(2):
            each(d, False, lambda d=d: back(d, c).start())

    def drain_hubs(ref, sem):
        @pl.when(mine_hub)
        def _():
            drain(ref, hubs - 1, sem)

        @pl.when(~mine_hub)
        def _():
            drain(ref, hubs, sem)

    stats = {}
    for c in range(heads):
        with jax.named_scope(f"w_halo{c}"):
            if c > 0:
                halo_wait(c, True)
            halo_wait(c, False)
        for b in range(nb):
            st = nt(listed_rows(0, c, b), stacked(qv, c, b))
            dp = nt(listed_rows(1, c, b), stacked(gv, c, b))
            top = jnp.max(st, axis=0, keepdims=True)
            ex = jnp.exp2((st - top) * fold)
            keep_ex[c, b] = ex
            keep_dp[c, b] = dp
            stats[c, b] = (
                top,
                jnp.sum(ex, axis=0, keepdims=True),
                jnp.sum(ex * dp, axis=0, keepdims=True),
            )
        if c == 0:
            with jax.named_scope("w_gall"):
                drain_hubs(gall, hr_sem.at[1])
        kg, vg = global_rows(gall, 0, c), global_rows(gall, 1, c)
        glob = [None, None]
        for b in range(nb):
            qs, gs = stacked(qv, c, b), stacked(gv, c, b)
            st = nt(kg, qs)
            dp = nt(vg, gs)
            top_w, sum_w, dot_w = stats[c, b]
            top = jnp.maximum(top_w, jnp.max(st, axis=0, keepdims=True))
            ex = jnp.exp2((st - top) * fold)
            shrink = jnp.exp2((top_w - top) * fold)
            inv = 1.0 / (sum_w * shrink + jnp.sum(ex, axis=0, keepdims=True))
            dot = (dot_w * shrink + jnp.sum(ex * dp, axis=0, keepdims=True)) * inv
            pr = ex * inv
            ds = (pr * (dp - dot)).astype(BF16)
            keep_ds[c, b] = ds
            stats[c, b] = (shrink * inv, dot)
            for t, part in enumerate((nn(ds, qs) * scale, nn(pr.astype(BF16), gs))):
                glob[t] = part if glob[t] is None else glob[t] + part
        for t in range(2):
            gpart[c, t] = glob[t].astype(BF16)

    for g in range(heads):
        @pl.when(me != hub_id(g))
        def _():
            remote(
                gpart.at[g], hub2_in.at[lane], hs_sem.at[2], hr_sem.at[2], hub_id(g)
            ).start()

    for c in range(heads):
        for b in range(nb):
            qs, gs = stacked(qv, c, b), stacked(gv, c, b)
            ratio, dot = stats[c, b]
            pr = keep_ex[c, b] * ratio
            ds = (pr * (keep_dp[c, b] - dot)).astype(BF16)
            dv = nn(pr.astype(BF16), gs)
            dk = nn(ds, qs) * scale
            for t, val in enumerate((dk, dv)):
                for l in range(listed):
                    wslot[b, l, t] = val[l * BLOCK : (l + 1) * BLOCK]
            ks = jnp.concatenate([listed_rows(0, c, b), global_rows(gall, 0, c)], axis=0)
            dqt = nn(ks.T, jnp.concatenate([ds, keep_ds[c, b]], axis=0)) * scale
            dq = dqt.T.astype(BF16)
            for i, s in enumerate(columns(c)):
                dq_ref[0, b * BLOCK : (b + 1) * BLOCK, s] = dq[i * BLOCK : (i + 1) * BLOCK]
        for dst in range(nb + 2 * REACH):
            total = None
            for b in range(nb):
                if not b <= dst <= b + 2 * REACH:
                    continue
                slot = jnp.int32(listed)
                for l in range(listed):
                    slot = jnp.where(local_idx[b][l] == dst, l, slot)
                term = wslot[b, slot]
                total = term if total is None else total + term
            if dst < REACH:
                sback[1, c, dst] = total.astype(BF16)
            elif dst < REACH + nb:
                own[c, dst - REACH] = total
            else:
                sback[0, c, dst - REACH - nb] = total.astype(BF16)
        with jax.named_scope(f"s_back{c}"):
            for d in range(2):
                each(d, False, lambda d=d, c=c: back(d, c).start())

    @pl.when(mine_hub)
    def _():
        with jax.named_scope("w_hub2"):
            drain(hub2_in, n // 2 - 1, hr_sem.at[2])
        hub2_in[lane] = gpart[group_of]
        half = jnp.sum(hub2_in[...].astype(F32), axis=0)
        cross_out[...] = half.astype(BF16)
        cross = remote(cross_out, cross_in, cross_sem.at[0], cross_sem.at[1], other_hub)
        cross.start()
        with jax.named_scope("w_cross"):
            cross.wait_recv()
        total = (half + cross_in[...].astype(F32)).astype(BF16)
        hub2_out[...] = total
        gall2[group_of] = total

        @pl.loop(1, n // 2)
        def _(k):
            q = lax.rem(lane + k, n // 2)
            target = (q // 2) * 4 + col * 2 + lax.rem(q, 2)
            remote(hub2_out, gall2.at[group_of], hs_sem.at[3], hr_sem.at[3], target).start()

        cross.wait_send()

    def drain_groups(ref, sem):
        @pl.when(mine_hub)
        def _():
            drain(ref, heads - 1, sem)

        @pl.when(~mine_hub)
        def _():
            drain(ref, heads, sem)

    with jax.named_scope("w_gall2"):
        drain_groups(gall2, hr_sem.at[3])

    flag = jnp.where(owner_ref[0] == me, 1.0, 0.0)
    for c in range(heads):
        with jax.named_scope(f'w_back{c}'):
            for d in range(2):
                each(d, True, lambda d=d, c=c: back(d, c).wait_recv())
        for t, out in enumerate((dk_ref, dv_ref)):
            extra = nn(hot, gall2[c, t]) * flag
            for i in range(nb):
                rsl = slice(i * BLOCK, (i + 1) * BLOCK)
                total = own[c, i, t] + extra[rsl]
                total = total + rback[0, c, i, t].astype(F32) + rback[1, c, i, t].astype(F32)
                out[0, rsl, c * DH : (c + 1) * DH] = total.astype(BF16)

    for c in range(heads):
        for d in range(2):
            for t in range(2):
                each(d, False, lambda d=d, c=c, t=t: halo(d, c, t).wait_send())
            each(d, False, lambda d=d, c=c: back(d, c).wait_send())

    @pl.when(mine_hub)
    def _():
        drain(hub_in, n - 1, hs_sem.at[1])
        drain(hub2_in, n // 2 - 1, hs_sem.at[3])

    drain_hubs(gsend, hs_sem.at[0])
    drain_groups(gpart, hs_sem.at[2])


def write_out(*refs):
    copies = [
        pltpu.make_async_copy(refs[i], refs[3 + i], refs[6].at[i]) for i in range(3)
    ]
    for cp in copies:
        cp.start()
    for cp in copies:
        cp.wait()


def solution(mesh):
    n = mesh.shape["seq"]

    def local(query, keys, values, grad_out, global_offset, owner, block_lists):
        rows, qw = query.shape[1:]
        kw = keys.shape[2]
        heads = kw // DH
        group = HQ // HK
        nb = rows // BLOCK
        listed = block_lists.shape[2]
        gtok = global_offset.shape[1]
        hubs = 2 * heads
        wide = nb + 2 * REACH
        assert nb == REACH and n % 8 == 0 and n >= 2 * hubs and heads % 2 == 0
        vm = pl.BlockSpec(memory_space=pltpu.VMEM)
        hb = pl.BlockSpec(memory_space=pl.ANY)
        held = pl.pallas_call(
            functools.partial(kernel, n, heads, group, nb, listed, gtok),
            out_shape=tuple(pltpu.VMEM(a.shape, BF16) for a in (query, keys, values)),
            in_specs=[hb] * 7,
            out_specs=(vm, vm, vm),
            scratch_shapes=[
                pltpu.SMEM(owner.shape, jnp.int32),
                pltpu.SMEM(block_lists.shape, jnp.int32),
                pltpu.VMEM(global_offset.shape, jnp.int32),
                pltpu.SemaphoreType.DMA((3,)),
                pltpu.VMEM((rows, qw), BF16),
                pltpu.VMEM((rows, qw), BF16),
                pltpu.VMEM((hubs, gtok, DH), BF16),
                pltpu.VMEM((n, gtok, DH), BF16),
                pltpu.VMEM((gtok, DH), BF16),
                pltpu.VMEM((hubs, gtok, DH), BF16),
                pltpu.VMEM((heads, 2, gtok, DH), BF16),
                pltpu.VMEM((n // 2, 2, gtok, DH), BF16),
                pltpu.VMEM((2, gtok, DH), BF16),
                pltpu.VMEM((2, gtok, DH), BF16),
                pltpu.VMEM((2, gtok, DH), BF16),
                pltpu.VMEM((heads, 2, gtok, DH), BF16),
                pltpu.SemaphoreType.DMA((2,)),
                pltpu.VMEM((heads, nb, listed * BLOCK, group * BLOCK), F32),
                pltpu.VMEM((heads, nb, listed * BLOCK, group * BLOCK), F32),
                pltpu.VMEM((heads, nb, gtok, group * BLOCK), BF16),
                pltpu.VMEM((nb, listed + 1, 2, BLOCK, DH), F32),
                pltpu.VMEM((heads, nb, 2, BLOCK, DH), F32),
                pltpu.VMEM((2, heads, REACH, 2, BLOCK, DH), BF16),
                pltpu.VMEM((2, heads, REACH, 2, BLOCK, DH), BF16),
                pltpu.SemaphoreType.DMA((2 * heads * nb,)),
                pltpu.SemaphoreType.DMA((2,)),
                pltpu.SemaphoreType.DMA((4 * heads,)),
                pltpu.SemaphoreType.DMA((4 * heads,)),
                pltpu.SemaphoreType.DMA((2 * heads,)),
                pltpu.SemaphoreType.DMA((2 * heads,)),
                pltpu.SemaphoreType.DMA((4,)),
                pltpu.SemaphoreType.DMA((4,)),
            ]
            + [pltpu.VMEM((wide, BLOCK, DH), BF16)] * (2 * heads),
            compiler_params=pltpu.CompilerParams(collective_id=0, has_side_effects=True),
        )(owner, block_lists, global_offset, query, keys, values, grad_out)
        return pl.pallas_call(
            write_out,
            out_shape=tuple(jax.ShapeDtypeStruct(a.shape, BF16) for a in (query, keys, values)),
            in_specs=[hb] * 3,
            out_specs=[hb] * 3,
            scratch_shapes=[pltpu.SemaphoreType.DMA((3,))],
        )(*[pltpu.with_memory_space_constraint(a, pltpu.VMEM) for a in held])

    return jax.shard_map(
        local,
        mesh=mesh,
        in_specs=(
            P(None, "seq", "head"),
            P(None, "seq", "head"),
            P(None, "seq", "head"),
            P(None, "seq", "head"),
            P(),
            P(),
            P(None, "seq", None),
        ),
        out_specs=(P(None, "seq", "head"), P(None, "seq", "head"), P(None, "seq", "head")),
        check_vma=False,
    )
```

```python
import functools

import jax
import jax.numpy as jnp
from jax import lax
from jax.experimental import pallas as pl
from jax.experimental.pallas import tpu as pltpu
from jax.sharding import PartitionSpec as P

HQ = 16
HK = 4
DH = 128
BLOCK = 128
REACH = 2
LOG2E = 1.4426950408889634
F32 = jnp.float32
BF16 = jnp.bfloat16


def nt(a, b):
    return lax.dot_general(a, b, (((1,), (1,)), ((), ())), preferred_element_type=F32)


def nn(a, b):
    return lax.dot_general(a, b, (((1,), (0,)), ((), ())), preferred_element_type=F32)


def kernel(
    n, heads, group, nb, listed, gtok,
    owner_hbm, lists_hbm, goff_hbm, q_hbm, k_hbm, v_hbm, g_hbm,
    dq_ref, dk_ref, dv_ref,
    owner_ref, lists_ref, goff_ref, small_sem, qv, gv, gsend, hub_in, hub_out, gcand, gall, fw_sem, gpart, hub2_in, cross_out, cross_in, hub2_out, gall2, cross_sem,
    keep_ex, keep_dp, keep_ds, wslot, own, sback, rback, load_sem, big_sem, ks_sem, kr_sem, gs_sem, gr_sem, hs_sem, hr_sem,
    *kvw,
):
    me = lax.axis_index("seq")
    hubs = 2 * heads
    rows = nb * BLOCK
    first = n // 2 - hubs + 1
    hub = (me - first) // 2
    col = lax.rem(me // 2, 2)
    lane = (me // 4) * 2 + lax.rem(me, 2)
    odd = lax.rem(me, 2) == 1
    level = hub // 2
    group_of = jnp.where(col == 0, level, heads - 1 - level)

    def row_of(g, side):
        return jnp.where(side == 0, g, heads - 1 - g)

    def hub_id(g, side):
        return first + 4 * row_of(g, side) + 2 * side

    def sum_id(g, side):
        return 4 * (g + side) + 2 * side + 1

    def is_adder(i):
        g = i // 4 - lax.rem(i // 2, 2)
        return (g >= 0) & (g < heads) & (lax.rem(i, 2) == 1)

    adder = is_adder(me)
    sum_group = jnp.clip(me // 4 - col, 0, heads - 1)
    other_sum = sum_id(sum_group, 1 - col)

    def hubbed(i):
        return (i >= first) & (i < first + 2 * hubs) & (lax.rem(i + first, 2) == 0)

    src_refs = (k_hbm, v_hbm)
    loads = []
    for t in range(2):
        for c in range(heads):
            for i in range(nb):
                cp = pltpu.make_async_copy(
                    src_refs[t].at[0, pl.ds(i * BLOCK, BLOCK), pl.ds(c * DH, DH)],
                    kvw[t * heads + c].at[REACH + i],
                    load_sem.at[(t * heads + c) * nb + i],
                )
                cp.start()
                loads.append(cp)
    small = [
        pltpu.make_async_copy(a, b, small_sem.at[i])
        for i, (a, b) in enumerate(
            ((goff_hbm, goff_ref), (owner_hbm, owner_ref), (lists_hbm, lists_ref))
        )
    ]
    for cp in small:
        cp.start()

    barrier = pltpu.get_barrier_semaphore()

    def greet(other):
        pl.semaphore_signal(
            barrier, inc=1, device_id={"seq": other}, device_id_type=pl.DeviceIdType.MESH
        )

    mine_hub = hubbed(me)

    @pl.when(mine_hub | adder)
    def _():
        @pl.loop(0, n // 2)
        def _(k):
            target = (k // 2) * 4 + col * 2 + lax.rem(k, 2)

            @pl.when((target != me) & (target != me - 1))
            def _():
                greet(target)

    @pl.when(odd)
    def _():
        for g in range(heads):
            greet(hub_id(g, 1 - col))

    @pl.when(adder & ~hubbed(other_sum))
    def _():
        greet(other_sum)

    @pl.when(me > 0)
    def _():
        greet(me - 1)

    @pl.when(me < n - 1)
    def _():
        greet(me + 1)

    cq = pltpu.make_async_copy(q_hbm.at[0], qv, big_sem.at[0])
    cg = pltpu.make_async_copy(g_hbm.at[0], gv, big_sem.at[1])

    with jax.named_scope("w_loads"):
        small[0].wait()
        for cp in loads:
            cp.wait()
    cq.start()
    cg.start()

    hot = lax.broadcasted_iota(jnp.int32, (rows, gtok), 0) == goff_ref[...]
    hot = jnp.where(hot, 1.0, 0.0).astype(BF16)
    for t in range(2):
        for c in range(heads):
            mine = kvw[t * heads + c][REACH : REACH + nb].reshape(rows, DH)
            got = lax.dot_general(hot, mine, (((0,), (0,)), ((), ())), preferred_element_type=F32)
            gsend[c, t] = got.astype(BF16)
    zeros_kv = jnp.zeros((REACH, BLOCK, DH), BF16)

    @pl.when(me == 0)
    def _():
        for ref in kvw:
            ref[0:REACH] = zeros_kv
        rback[0] = jnp.zeros(rback.shape[1:], BF16)

    @pl.when(me == n - 1)
    def _():
        for ref in kvw:
            ref[REACH + nb : REACH + nb + REACH] = zeros_kv
        rback[1] = jnp.zeros(rback.shape[1:], BF16)

    zero_tile = jnp.zeros((nb, 2, BLOCK, DH), F32)
    wslot[:, listed] = zero_tile

    def served(i):
        return jnp.where(hubbed(i) | is_adder(i), 1, 0)

    beside = jnp.where(me > 0, 1, 0) + jnp.where(me < n - 1, 1, 0)
    callers = sum(
        jnp.where(is_adder(hub_id(g, col)), 0, 1) for g in range(heads)
    ) + heads
    greeted = callers - served(me) - jnp.where(odd, 0, served(me + 1))
    greeted = greeted + jnp.where(mine_hub, n // 4, 0) + jnp.where(adder & ~mine_hub, 1, 0)
    with jax.named_scope("w_barrier"):
        pl.semaphore_wait(barrier, beside + greeted)

    def remote(src, dst, s_sem, r_sem, target):
        return pltpu.make_async_remote_copy(
            src_ref=src, dst_ref=dst, send_sem=s_sem, recv_sem=r_sem,
            device_id={"seq": target}, device_id_type=pl.DeviceIdType.MESH,
        )

    def to_hub(src, dst, i, g, target):
        @pl.when(me != target)
        def _():
            remote(src.at[g], dst.at[lane], hs_sem.at[i], hr_sem.at[i], target).start()

    def drain(ref, count, sem):
        part = ref.at[pl.ds(0, count)]
        pltpu.make_async_copy(part, part, sem).wait()

    for g in range(heads):
        to_hub(gsend, hub_in, 0, g, hub_id(g, col))

    def halo(direction, c, t):
        idx = (direction * heads + c) * 2 + t
        ref = kvw[t * heads + c]
        if direction == 0:
            src, dst, target = ref.at[pl.ds(nb, REACH)], ref.at[pl.ds(0, REACH)], me + 1
        else:
            src, dst, target = ref.at[pl.ds(REACH, REACH)], ref.at[pl.ds(REACH + nb, REACH)], me - 1
        return remote(src, dst, ks_sem.at[idx], kr_sem.at[idx], target)

    def back(direction, c):
        idx = direction * heads + c
        target = me + 1 if direction == 0 else me - 1
        return remote(
            sback.at[direction, c], rback.at[direction, c], gs_sem.at[idx], gr_sem.at[idx], target
        )

    def each(direction, receiving, what):
        up = (direction == 0) != receiving
        cond = me < n - 1 if up else me > 0
        pl.when(cond)(what)

    place = lax.rem(me, 4)

    def far(d):
        return place == (3 if d == 0 else 0)

    def halo_start(c, d, late):
        for t in range(2):
            cond = (me < n - 1 if d == 0 else me > 0) & (far(d) if late else ~far(d))
            pl.when(cond)(lambda t=t: halo(d, c, t).start())

    held = mine_hub & (place == 1)

    halo_start(0, 0, False)
    halo_start(0, 1, False)
    for c in range(1, heads):
        halo_start(c, 1, False)
        pl.when(~held)(functools.partial(halo_start, c, 0, False))
    for c in range(heads):
        for d in range(2):
            halo_start(c, d, True)

    def halo_wait(c, paired):
        for d in range(2):
            cond = (me > 0 if d == 0 else me < n - 1) & ((odd if d == 0 else ~odd) == paired)
            for t in range(2):
                pl.when(cond)(lambda d=d, t=t: halo(d, c, t).wait_recv())

    for cp in small[1:]:
        cp.wait()

    with jax.named_scope('w_qg'):
        cq.wait()
        cg.wait()
    scale = DH ** (-0.5)
    fold = scale * LOG2E
    local_idx = [
        [
            jnp.clip(lists_ref[0, b, l] - me * nb + REACH, 0, nb + 2 * REACH - 1)
            for l in range(listed)
        ]
        for b in range(nb)
    ]

    def near_rows(t, c, b):
        return [kvw[t * heads + c][local_idx[b][l]] for l in range(1, listed)]

    def columns(c):
        return [slice((c * group + i) * DH, (c * group + i + 1) * DH) for i in range(group)]

    def stacked(ref, c, b):
        rsl = slice(b * BLOCK, (b + 1) * BLOCK)
        return jnp.concatenate([ref[rsl, s] for s in columns(c)], axis=0)

    def logits(ks, vs, c, b):
        return nt(ks, stacked(qv, c, b)), nt(vs, stacked(gv, c, b))

    def keep(c, b, start, st, dp):
        top = jnp.max(st, axis=0, keepdims=True)
        ex = jnp.exp2((st - top) * fold)
        keep_ex[c, b, start : start + st.shape[0]] = ex
        keep_dp[c, b, start : start + st.shape[0]] = dp
        total = jnp.sum(ex, axis=0, keepdims=True)
        return top, total, jnp.sum(ex * dp, axis=0, keepdims=True)

    window = listed * BLOCK
    stats = {}
    for c in range(heads):
        for b in range(nb):
            kb, vb = kvw[c][REACH + b], kvw[heads + c][REACH + b]
            stats[c, b] = [keep(c, b, 0, *logits(kb, vb, c, b))]

    def far_first(i, count):
        return jnp.where(lax.rem(i, 2) == 0, count - 1 - i // 2, i // 2)

    owner_at = owner_ref[0]

    @pl.when(mine_hub)
    def _():
        with jax.named_scope("w_hub1"):
            drain(hub_in, n // 2 - 1, hr_sem.at[0])
        hub_in[lane] = gsend[group_of]
        pick = hub_in[(owner_at // 4) * 2 + lax.rem(owner_at, 2)]
        hub_out[...] = pick
        gcand[col * heads + group_of] = pick

        @pl.loop(0, n // 2)
        def _(k):
            target = 4 * far_first(k // 2, n // 4) + 2 * lax.rem(k, 2) + 1

            @pl.when(target != me)
            def _():
                remote(
                    hub_out, gcand.at[col * heads + group_of], hs_sem.at[1], hr_sem.at[1], target
                ).start()

        @pl.when(held)
        def _():
            for c in range(1, heads):
                halo_start(c, 0, False)

    def back_start(c):
        for d in range(2):
            each(d, False, lambda d=d: back(d, c).start())

    def drain_own(ref, count, sem, self_served):
        @pl.when(self_served)
        def _():
            drain(ref, count - 1, sem)

        @pl.when(~self_served)
        def _():
            drain(ref, count, sem)

    pass_on = remote(gall, gall, fw_sem.at[0], fw_sem.at[1], jnp.where(odd, me - 1, me + 1))

    def collect():
        with jax.named_scope("w_cand"):
            drain_own(gcand, 2 * heads, hr_sem.at[1], mine_hub)
        side = lax.rem(owner_at // 2, 2) * heads
        for g in range(heads):
            gall[g] = gcand[side + g]
        pass_on.start()

    ratios = {}
    for c in range(heads):
        last = c == heads - 1
        with jax.named_scope(f"w_halo{c}"):
            halo_wait(c, True)
            halo_wait(c, False)
        if not last:
            for b in range(nb):
                kn = jnp.concatenate(near_rows(0, c, b), axis=0)
                vn = jnp.concatenate(near_rows(1, c, b), axis=0)
                stats[c, b].append(keep(c, b, BLOCK, *logits(kn, vn, c, b)))
        if c == 0:
            pl.when(odd)(collect)
            with jax.named_scope("w_gall"):
                @pl.when(~odd)
                def _():
                    pass_on.wait_recv()
        glob = [None, None]
        for b in range(nb):
            qs, gs = stacked(qv, c, b), stacked(gv, c, b)
            kn, vn = [gall[c, 0]], [gall[c, 1]]
            if last:
                kn, vn = near_rows(0, c, b) + kn, near_rows(1, c, b) + vn
            st, dp = logits(jnp.concatenate(kn, axis=0), jnp.concatenate(vn, axis=0), c, b)
            top = jnp.max(st, axis=0, keepdims=True)
            for old in stats[c, b]:
                top = jnp.maximum(top, old[0])
            ex = jnp.exp2((st - top) * fold)
            total = jnp.sum(ex, axis=0, keepdims=True)
            dot = jnp.sum(ex * dp, axis=0, keepdims=True)
            shrinks = [jnp.exp2((old[0] - top) * fold) for old in stats[c, b]]
            for shrink, old in zip(shrinks, stats[c, b]):
                total = total + old[1] * shrink
                dot = dot + old[2] * shrink
            inv = 1.0 / total
            dot = dot * inv
            if last:
                near = window - BLOCK
                keep_ex[c, b, BLOCK:window] = ex[:near]
                keep_dp[c, b, BLOCK:window] = dp[:near]
                ex, dp = ex[near:], dp[near:]
            pr = ex * inv
            ds = (pr * (dp - dot)).astype(BF16)
            keep_ds[c, b, window:] = ds
            own_ratio = shrinks[0] * inv
            ratios[c, b] = (own_ratio, inv if last else shrinks[1] * inv, dot)
            for t, part in enumerate((nn(ds, qs) * scale, nn(pr.astype(BF16), gs))):
                glob[t] = part if glob[t] is None else glob[t] + part
        for t in range(2):
            gpart[c, t] = glob[t].astype(BF16)
        with jax.named_scope(f"s_gpart{c}"):
            to_hub(gpart, hub2_in, 2, c, sum_id(c, col))

    for c in range(heads):
        for b in range(nb):
            qs, gs = stacked(qv, c, b), stacked(gv, c, b)
            own_ratio, near_ratio, dot = ratios[c, b]
            vals = []
            for lo, hi, ratio in ((0, BLOCK, own_ratio), (BLOCK, window, near_ratio)):
                pr = keep_ex[c, b, lo:hi] * ratio
                ds = (pr * (keep_dp[c, b, lo:hi] - dot)).astype(BF16)
                keep_ds[c, b, lo:hi] = ds
                vals.append((ds, pr.astype(BF16)))
            ds, pr = (jnp.concatenate([v[i] for v in vals], axis=0) for i in range(2))
            for t, val in enumerate((nn(ds, qs) * scale, nn(pr, gs))):
                for l in range(listed):
                    wslot[b, l, t] = val[l * BLOCK : (l + 1) * BLOCK]
        for dst in range(nb + 2 * REACH):
            total = None
            for b in range(nb):
                if not b <= dst <= b + 2 * REACH:
                    continue
                slot = jnp.int32(listed)
                for l in range(1, listed):
                    slot = jnp.where(local_idx[b][l] == dst, l, slot)
                term = wslot[b, 0] if dst == b + REACH else wslot[b, slot]
                total = term if total is None else total + term
            if dst < REACH:
                sback[1, c, dst] = total.astype(BF16)
            elif dst < REACH + nb:
                own[c, dst - REACH] = total
            else:
                sback[0, c, dst - REACH - nb] = total.astype(BF16)
        with jax.named_scope(f"s_back{c}"):
            back_start(c)

    for c in range(heads):
        for b in range(nb):
            ks = jnp.concatenate([kvw[c][REACH + b]] + near_rows(0, c, b) + [gall[c, 0]], axis=0)
            dqt = nn(ks.T, keep_ds[c, b]) * scale
            dq = dqt.T.astype(BF16)
            for i, s in enumerate(columns(c)):
                dq_ref[0, b * BLOCK : (b + 1) * BLOCK, s] = dq[i * BLOCK : (i + 1) * BLOCK]

    @pl.when(adder)
    def _():
        with jax.named_scope("w_hub2"):
            drain(hub2_in, n // 2 - 1, hr_sem.at[2])
        hub2_in[lane] = gpart[sum_group]
        half = jnp.sum(hub2_in[...].astype(F32), axis=0)
        cross_out[...] = half.astype(BF16)
        cross = remote(cross_out, cross_in, cross_sem.at[0], cross_sem.at[1], other_sum)
        cross.start()
        with jax.named_scope("w_cross"):
            cross.wait_recv()
        total = (half + cross_in[...].astype(F32)).astype(BF16)
        hub2_out[...] = total
        gall2[sum_group] = total

        @pl.loop(0, n // 2)
        def _(k):
            target = 4 * far_first(k // 2, n // 4) + col * 2 + lax.rem(k, 2)

            @pl.when(target != me)
            def _():
                remote(
                    hub2_out, gall2.at[sum_group], hs_sem.at[3], hr_sem.at[3], target
                ).start()

        cross.wait_send()

    for c in range(heads):
        with jax.named_scope(f"w_back{c}"):
            for d in range(2):
                each(d, True, lambda d=d, c=c: back(d, c).wait_recv())
        for t in range(2):
            for i in range(nb):
                total = rback[0, c, i, t].astype(F32) + rback[1, c, i, t].astype(F32)
                own[c, i, t] = own[c, i, t] + total

    with jax.named_scope("w_gall2"):
        drain_own(gall2, heads, hr_sem.at[3], adder)

    flag = jnp.where(owner_ref[0] == me, 1.0, 0.0)
    for c in range(heads):
        for t, out in enumerate((dk_ref, dv_ref)):
            extra = nn(hot, gall2[c, t]) * flag
            for i in range(nb):
                rsl = slice(i * BLOCK, (i + 1) * BLOCK)
                out[0, rsl, c * DH : (c + 1) * DH] = (own[c, i, t] + extra[rsl]).astype(BF16)

    for c in range(heads):
        for d in range(2):
            for t in range(2):
                each(d, False, lambda d=d, c=c, t=t: halo(d, c, t).wait_send())
            each(d, False, lambda d=d, c=c: back(d, c).wait_send())

    @pl.when(odd)
    def _():
        pass_on.wait_send()

    @pl.when(mine_hub)
    def _():
        drain(hub_in, n // 2 - 1, hs_sem.at[1])

    @pl.when(adder)
    def _():
        drain(hub2_in, n // 2 - 1, hs_sem.at[3])

    drain_own(gsend, heads, hs_sem.at[0], mine_hub)
    drain_own(gpart, heads, hs_sem.at[2], adder)


def write_out(*refs):
    copies = [
        pltpu.make_async_copy(refs[i], refs[3 + i], refs[6].at[i]) for i in range(3)
    ]
    for cp in copies:
        cp.start()
    for cp in copies:
        cp.wait()


def solution(mesh):
    n = mesh.shape["seq"]

    def local(query, keys, values, grad_out, global_offset, owner, block_lists):
        rows, qw = query.shape[1:]
        kw = keys.shape[2]
        heads = kw // DH
        group = HQ // HK
        nb = rows // BLOCK
        listed = block_lists.shape[2]
        gtok = global_offset.shape[1]
        hubs = 2 * heads
        wide = nb + 2 * REACH
        assert nb == REACH and n % 8 == 0 and n >= 2 * hubs and heads % 2 == 0
        vm = pl.BlockSpec(memory_space=pltpu.VMEM)
        hb = pl.BlockSpec(memory_space=pl.ANY)
        held = pl.pallas_call(
            functools.partial(kernel, n, heads, group, nb, listed, gtok),
            out_shape=tuple(pltpu.VMEM(a.shape, BF16) for a in (query, keys, values)),
            in_specs=[hb] * 7,
            out_specs=(vm, vm, vm),
            scratch_shapes=[
                pltpu.SMEM(owner.shape, jnp.int32),
                pltpu.SMEM(block_lists.shape, jnp.int32),
                pltpu.VMEM(global_offset.shape, jnp.int32),
                pltpu.SemaphoreType.DMA((3,)),
                pltpu.VMEM((rows, qw), BF16),
                pltpu.VMEM((rows, qw), BF16),
                pltpu.VMEM((heads, 2, gtok, DH), BF16),
                pltpu.VMEM((n // 2, 2, gtok, DH), BF16),
                pltpu.VMEM((2, gtok, DH), BF16),
                pltpu.VMEM((2 * heads, 2, gtok, DH), BF16),
                pltpu.VMEM((heads, 2, gtok, DH), BF16),
                pltpu.SemaphoreType.DMA((2,)),
                pltpu.VMEM((heads, 2, gtok, DH), BF16),
                pltpu.VMEM((n // 2, 2, gtok, DH), BF16),
                pltpu.VMEM((2, gtok, DH), BF16),
                pltpu.VMEM((2, gtok, DH), BF16),
                pltpu.VMEM((2, gtok, DH), BF16),
                pltpu.VMEM((heads, 2, gtok, DH), BF16),
                pltpu.SemaphoreType.DMA((2,)),
                pltpu.VMEM((heads, nb, listed * BLOCK, group * BLOCK), F32),
                pltpu.VMEM((heads, nb, listed * BLOCK, group * BLOCK), F32),
                pltpu.VMEM((heads, nb, listed * BLOCK + gtok, group * BLOCK), BF16),
                pltpu.VMEM((nb, listed + 1, 2, BLOCK, DH), F32),
                pltpu.VMEM((heads, nb, 2, BLOCK, DH), F32),
                pltpu.VMEM((2, heads, REACH, 2, BLOCK, DH), BF16),
                pltpu.VMEM((2, heads, REACH, 2, BLOCK, DH), BF16),
                pltpu.SemaphoreType.DMA((2 * heads * nb,)),
                pltpu.SemaphoreType.DMA((2,)),
                pltpu.SemaphoreType.DMA((4 * heads,)),
                pltpu.SemaphoreType.DMA((4 * heads,)),
                pltpu.SemaphoreType.DMA((2 * heads,)),
                pltpu.SemaphoreType.DMA((2 * heads,)),
                pltpu.SemaphoreType.DMA((4,)),
                pltpu.SemaphoreType.DMA((4,)),
            ]
            + [pltpu.VMEM((wide, BLOCK, DH), BF16)] * (2 * heads),
            compiler_params=pltpu.CompilerParams(collective_id=0, has_side_effects=True),
        )(owner, block_lists, global_offset, query, keys, values, grad_out)
        return pl.pallas_call(
            write_out,
            out_shape=tuple(jax.ShapeDtypeStruct(a.shape, BF16) for a in (query, keys, values)),
            in_specs=[hb] * 3,
            out_specs=[hb] * 3,
            scratch_shapes=[pltpu.SemaphoreType.DMA((3,))],
        )(*[pltpu.with_memory_space_constraint(a, pltpu.VMEM) for a in held])

    return jax.shard_map(
        local,
        mesh=mesh,
        in_specs=(
            P(None, "seq", "head"),
            P(None, "seq", "head"),
            P(None, "seq", "head"),
            P(None, "seq", "head"),
            P(),
            P(),
            P(None, "seq", None),
        ),
        out_specs=(P(None, "seq", "head"), P(None, "seq", "head"), P(None, "seq", "head")),
        check_vma=False,
    )
```

```python
import functools

import jax
import jax.numpy as jnp
from jax import lax
from jax.experimental import pallas as pl
from jax.experimental.pallas import tpu as pltpu
from jax.sharding import PartitionSpec as P

HQ = 16
HK = 4
DH = 128
BLOCK = 128
REACH = 2
LEADS = 2
LOG2E = 1.4426950408889634
F32 = jnp.float32
BF16 = jnp.bfloat16


def nt(a, b):
    return lax.dot_general(a, b, (((1,), (1,)), ((), ())), preferred_element_type=F32)


def nn(a, b):
    return lax.dot_general(a, b, (((1,), (0,)), ((), ())), preferred_element_type=F32)


def kernel(
    n, heads, group, nb, listed, gtok,
    owner_hbm, lists_hbm, goff_hbm, q_hbm, k_hbm, v_hbm, g_hbm,
    dq_ref, dk_ref, dv_ref,
    owner_ref, lists_ref, goff_ref, small_sem, qv, gv, gsend, hub_in, hub_out, gcand, gall, fw_sem, gpart, hub2_in, half_out, total_out, cross_in, sums, cross_sem,
    keep_ex, keep_dp, keep_ds, wslot, own, sback, rback, load_sem, big_sem, ks_sem, kr_sem, gs_sem, gr_sem, hs_sem, hr_sem,
    *kvw,
):
    me = lax.axis_index("seq")
    hubs = 2 * heads
    rows = nb * BLOCK
    first = n // 2 - hubs + 1
    hub = (me - first) // 2
    col = lax.rem(me // 2, 2)
    lane = (me // 4) * 2 + lax.rem(me, 2)
    odd = lax.rem(me, 2) == 1
    level = hub // 2
    group_of = jnp.where(col == 0, level, heads - 1 - level)

    def row_of(g, side):
        return jnp.where(side == 0, g, heads - 1 - g)

    def hub_id(g, side):
        return first + 4 * row_of(g, side) + 2 * side

    def sum_id(g, side):
        return 4 * (g + side) + 2 * side + 1

    def is_adder(i):
        g = i // 4 - lax.rem(i // 2, 2)
        return (g >= 0) & (g < heads) & (lax.rem(i, 2) == 1)

    adder = is_adder(me)
    sum_group = jnp.clip(me // 4 - col, 0, heads - 1)
    other_sum = sum_id(sum_group, 1 - col)

    def hubbed(i):
        return (i >= first) & (i < first + 2 * hubs) & (lax.rem(i + first, 2) == 0)

    src_refs = (k_hbm, v_hbm)
    loads = []
    for t in range(2):
        for c in range(heads):
            for i in range(nb):
                cp = pltpu.make_async_copy(
                    src_refs[t].at[0, pl.ds(i * BLOCK, BLOCK), pl.ds(c * DH, DH)],
                    kvw[t * heads + c].at[REACH + i],
                    load_sem.at[(t * heads + c) * nb + i],
                )
                cp.start()
                loads.append(cp)
    small = [
        pltpu.make_async_copy(a, b, small_sem.at[i])
        for i, (a, b) in enumerate(
            ((goff_hbm, goff_ref), (owner_hbm, owner_ref), (lists_hbm, lists_ref))
        )
    ]
    for cp in small:
        cp.start()

    barrier = pltpu.get_barrier_semaphore()

    def greet(other):
        pl.semaphore_signal(
            barrier, inc=1, device_id={"seq": other}, device_id_type=pl.DeviceIdType.MESH
        )

    mine_hub = hubbed(me)

    @pl.when(mine_hub)
    def _():
        @pl.loop(0, n // 2)
        def _(k):
            target = (k // 2) * 4 + col * 2 + lax.rem(k, 2)

            @pl.when((target != me) & (target != me - 1))
            def _():
                greet(target)

    @pl.when(odd)
    def _():
        for g in range(heads):
            greet(hub_id(g, 1 - col))

    @pl.when(me > 0)
    def _():
        greet(me - 1)

    @pl.when(me < n - 1)
    def _():
        greet(me + 1)

    cq = pltpu.make_async_copy(q_hbm.at[0], qv, big_sem.at[0])
    cg = pltpu.make_async_copy(g_hbm.at[0], gv, big_sem.at[1])

    with jax.named_scope("w_loads"):
        small[0].wait()
        for cp in loads:
            cp.wait()
    cq.start()
    cg.start()

    hot = lax.broadcasted_iota(jnp.int32, (rows, gtok), 0) == goff_ref[...]
    hot = jnp.where(hot, 1.0, 0.0).astype(BF16)
    for t in range(2):
        for c in range(heads):
            mine = kvw[t * heads + c][REACH : REACH + nb].reshape(rows, DH)
            got = lax.dot_general(hot, mine, (((0,), (0,)), ((), ())), preferred_element_type=F32)
            gsend[c, t] = got.astype(BF16)
    zeros_kv = jnp.zeros((REACH, BLOCK, DH), BF16)

    @pl.when(me == 0)
    def _():
        for ref in kvw:
            ref[0:REACH] = zeros_kv
        rback[0] = jnp.zeros(rback.shape[1:], BF16)

    @pl.when(me == n - 1)
    def _():
        for ref in kvw:
            ref[REACH + nb : REACH + nb + REACH] = zeros_kv
        rback[1] = jnp.zeros(rback.shape[1:], BF16)

    lead = me < LEADS
    no_sum = jnp.zeros((2, gtok, DH), BF16)
    for g in range(heads):
        @pl.when(~lead | (adder & (sum_group == g)))
        def _():
            sums[heads + g] = no_sum

    zero_tile = jnp.zeros((nb, 2, BLOCK, DH), F32)
    wslot[:, listed] = zero_tile

    beside = jnp.where(me > 0, 1, 0) + jnp.where(me < n - 1, 1, 0)
    greeted = heads + jnp.where(mine_hub, n // 4 - 1, 0) - jnp.where(hubbed(me + 1), 1, 0)
    with jax.named_scope("w_barrier"):
        pl.semaphore_wait(barrier, beside + greeted)

    def remote(src, dst, s_sem, r_sem, target):
        return pltpu.make_async_remote_copy(
            src_ref=src, dst_ref=dst, send_sem=s_sem, recv_sem=r_sem,
            device_id={"seq": target}, device_id_type=pl.DeviceIdType.MESH,
        )

    def to_hub(src, dst, i, g, target):
        @pl.when(me != target)
        def _():
            remote(src.at[g], dst.at[lane], hs_sem.at[i], hr_sem.at[i], target).start()

    def drain(ref, count, sem):
        part = ref.at[pl.ds(0, count)]
        pltpu.make_async_copy(part, part, sem).wait()

    for g in range(heads):
        to_hub(gsend, hub_in, 0, g, hub_id(g, col))

    def halo(direction, c, t):
        idx = (direction * heads + c) * 2 + t
        ref = kvw[t * heads + c]
        if direction == 0:
            src, dst, target = ref.at[pl.ds(nb, REACH)], ref.at[pl.ds(0, REACH)], me + 1
        else:
            src, dst, target = ref.at[pl.ds(REACH, REACH)], ref.at[pl.ds(REACH + nb, REACH)], me - 1
        return remote(src, dst, ks_sem.at[idx], kr_sem.at[idx], target)

    def back(direction, c):
        idx = direction * heads + c
        target = me + 1 if direction == 0 else me - 1
        return remote(
            sback.at[direction, c], rback.at[direction, c], gs_sem.at[idx], gr_sem.at[idx], target
        )

    def each(direction, receiving, what):
        up = (direction == 0) != receiving
        cond = me < n - 1 if up else me > 0
        pl.when(cond)(what)

    place = lax.rem(me, 4)

    def far(d):
        return place == (3 if d == 0 else 0)

    def halo_start(c, d, late):
        for t in range(2):
            cond = (me < n - 1 if d == 0 else me > 0) & (far(d) if late else ~far(d))
            pl.when(cond)(lambda t=t: halo(d, c, t).start())

    held = mine_hub & (place == 1)

    halo_start(0, 0, False)
    halo_start(0, 1, False)
    for c in range(1, heads):
        halo_start(c, 1, False)
        pl.when(~held)(functools.partial(halo_start, c, 0, False))
    for c in range(heads):
        for d in range(2):
            halo_start(c, d, True)

    def halo_wait(c, paired):
        for d in range(2):
            cond = (me > 0 if d == 0 else me < n - 1) & ((odd if d == 0 else ~odd) == paired)
            for t in range(2):
                pl.when(cond)(lambda d=d, t=t: halo(d, c, t).wait_recv())

    for cp in small[1:]:
        cp.wait()

    with jax.named_scope('w_qg'):
        cq.wait()
        cg.wait()
    scale = DH ** (-0.5)
    fold = scale * LOG2E
    local_idx = [
        [
            jnp.clip(lists_ref[0, b, l] - me * nb + REACH, 0, nb + 2 * REACH - 1)
            for l in range(listed)
        ]
        for b in range(nb)
    ]

    def near_rows(t, c, b):
        return [kvw[t * heads + c][local_idx[b][l]] for l in range(1, listed)]

    def columns(c):
        return [slice((c * group + i) * DH, (c * group + i + 1) * DH) for i in range(group)]

    def stacked(ref, c, b):
        rsl = slice(b * BLOCK, (b + 1) * BLOCK)
        return jnp.concatenate([ref[rsl, s] for s in columns(c)], axis=0)

    def logits(ks, vs, c, b):
        return nt(ks, stacked(qv, c, b)), nt(vs, stacked(gv, c, b))

    def keep(c, b, start, st, dp):
        top = jnp.max(st, axis=0, keepdims=True)
        ex = jnp.exp2((st - top) * fold)
        keep_ex[c, b, start : start + st.shape[0]] = ex
        keep_dp[c, b, start : start + st.shape[0]] = dp
        total = jnp.sum(ex, axis=0, keepdims=True)
        return top, total, jnp.sum(ex * dp, axis=0, keepdims=True)

    window = listed * BLOCK
    stats = {}
    for c in range(heads):
        for b in range(nb):
            kb, vb = kvw[c][REACH + b], kvw[heads + c][REACH + b]
            stats[c, b] = [keep(c, b, 0, *logits(kb, vb, c, b))]

    def far_first(i, count):
        return jnp.where(lax.rem(i, 2) == 0, count - 1 - i // 2, i // 2)

    owner_at = owner_ref[0]

    @pl.when(mine_hub)
    def _():
        with jax.named_scope("w_hub1"):
            drain(hub_in, n // 2 - 1, hr_sem.at[0])
        hub_in[lane] = gsend[group_of]
        pick = hub_in[(owner_at // 4) * 2 + lax.rem(owner_at, 2)]
        hub_out[...] = pick
        gcand[col * heads + group_of] = pick

        @pl.loop(0, n // 2)
        def _(k):
            target = 4 * far_first(k // 2, n // 4) + 2 * lax.rem(k, 2) + 1

            @pl.when(target != me)
            def _():
                remote(
                    hub_out, gcand.at[col * heads + group_of], hs_sem.at[1], hr_sem.at[1], target
                ).start()

        @pl.when(held)
        def _():
            for c in range(1, heads):
                halo_start(c, 0, False)

    def back_start(c):
        for d in range(2):
            each(d, False, lambda d=d: back(d, c).start())

    def drain_own(ref, count, sem, self_served):
        @pl.when(self_served)
        def _():
            drain(ref, count - 1, sem)

        @pl.when(~self_served)
        def _():
            drain(ref, count, sem)

    pass_on = remote(gall, gall, fw_sem.at[0], fw_sem.at[1], jnp.where(odd, me - 1, me + 1))

    def collect():
        with jax.named_scope("w_cand"):
            drain_own(gcand, 2 * heads, hr_sem.at[1], mine_hub)
        side = lax.rem(owner_at // 2, 2) * heads
        for g in range(heads):
            gall[g] = gcand[side + g]
        pass_on.start()

    ratios = {}
    for c in range(heads):
        last = c == heads - 1
        with jax.named_scope(f"w_halo{c}"):
            halo_wait(c, True)
            halo_wait(c, False)
        if not last:
            for b in range(nb):
                kn = jnp.concatenate(near_rows(0, c, b), axis=0)
                vn = jnp.concatenate(near_rows(1, c, b), axis=0)
                stats[c, b].append(keep(c, b, BLOCK, *logits(kn, vn, c, b)))
        if c == 0:
            pl.when(odd)(collect)
            with jax.named_scope("w_gall"):
                @pl.when(~odd)
                def _():
                    pass_on.wait_recv()
        glob = [None, None]
        for b in range(nb):
            qs, gs = stacked(qv, c, b), stacked(gv, c, b)
            kn, vn = [gall[c, 0]], [gall[c, 1]]
            if last:
                kn, vn = near_rows(0, c, b) + kn, near_rows(1, c, b) + vn
            st, dp = logits(jnp.concatenate(kn, axis=0), jnp.concatenate(vn, axis=0), c, b)
            top = jnp.max(st, axis=0, keepdims=True)
            for old in stats[c, b]:
                top = jnp.maximum(top, old[0])
            ex = jnp.exp2((st - top) * fold)
            total = jnp.sum(ex, axis=0, keepdims=True)
            dot = jnp.sum(ex * dp, axis=0, keepdims=True)
            shrinks = [jnp.exp2((old[0] - top) * fold) for old in stats[c, b]]
            for shrink, old in zip(shrinks, stats[c, b]):
                total = total + old[1] * shrink
                dot = dot + old[2] * shrink
            inv = 1.0 / total
            dot = dot * inv
            if last:
                near = window - BLOCK
                keep_ex[c, b, BLOCK:window] = ex[:near]
                keep_dp[c, b, BLOCK:window] = dp[:near]
                ex, dp = ex[near:], dp[near:]
            pr = ex * inv
            ds = (pr * (dp - dot)).astype(BF16)
            keep_ds[c, b, window:] = ds
            own_ratio = shrinks[0] * inv
            ratios[c, b] = (own_ratio, inv if last else shrinks[1] * inv, dot)
            for t, part in enumerate((nn(ds, qs) * scale, nn(pr.astype(BF16), gs))):
                glob[t] = part if glob[t] is None else glob[t] + part
        for t in range(2):
            gpart[c, t] = glob[t].astype(BF16)
        with jax.named_scope(f"s_gpart{c}"):
            to_hub(gpart, hub2_in, 2, c, sum_id(c, col))

    for c in range(heads):
        for b in range(nb):
            qs, gs = stacked(qv, c, b), stacked(gv, c, b)
            own_ratio, near_ratio, dot = ratios[c, b]
            vals = []
            for lo, hi, ratio in ((0, BLOCK, own_ratio), (BLOCK, window, near_ratio)):
                pr = keep_ex[c, b, lo:hi] * ratio
                ds = (pr * (keep_dp[c, b, lo:hi] - dot)).astype(BF16)
                keep_ds[c, b, lo:hi] = ds
                vals.append((ds, pr.astype(BF16)))
            ds, pr = (jnp.concatenate([v[i] for v in vals], axis=0) for i in range(2))
            for t, val in enumerate((nn(ds, qs) * scale, nn(pr, gs))):
                for l in range(listed):
                    wslot[b, l, t] = val[l * BLOCK : (l + 1) * BLOCK]
        for dst in range(nb + 2 * REACH):
            total = None
            for b in range(nb):
                if not b <= dst <= b + 2 * REACH:
                    continue
                slot = jnp.int32(listed)
                for l in range(1, listed):
                    slot = jnp.where(local_idx[b][l] == dst, l, slot)
                term = wslot[b, 0] if dst == b + REACH else wslot[b, slot]
                total = term if total is None else total + term
            if dst < REACH:
                sback[1, c, dst] = total.astype(BF16)
            elif dst < REACH + nb:
                own[c, dst - REACH] = total
            else:
                sback[0, c, dst - REACH - nb] = total.astype(BF16)
        with jax.named_scope(f"s_back{c}"):
            back_start(c)

    for c in range(heads):
        for b in range(nb):
            ks = jnp.concatenate([kvw[c][REACH + b]] + near_rows(0, c, b) + [gall[c, 0]], axis=0)
            dqt = nn(ks.T, keep_ds[c, b]) * scale
            dq = dqt.T.astype(BF16)
            for i, s in enumerate(columns(c)):
                dq_ref[0, b * BLOCK : (b + 1) * BLOCK, s] = dq[i * BLOCK : (i + 1) * BLOCK]

    def give(src, target, at):
        remote(src, sums.at[at], hs_sem.at[3], hr_sem.at[3], target).start()

    @pl.when(adder)
    def _():
        with jax.named_scope("w_hub2"):
            drain(hub2_in, n // 2 - 1, hr_sem.at[2])
        hub2_in[lane] = gpart[sum_group]
        half = jnp.sum(hub2_in[...].astype(F32), axis=0)
        half_out[...] = half.astype(BF16)
        cross = remote(half_out, cross_in, cross_sem.at[0], cross_sem.at[1], other_sum)
        cross.start()
        for target in range(LEADS):
            @pl.when((me != target) & (other_sum != target))
            def _():
                give(half_out, target, col * heads + sum_group)

        with jax.named_scope("w_cross"):
            cross.wait_recv()
        total = (half + cross_in[...].astype(F32)).astype(BF16)
        total_out[...] = total
        sums[sum_group] = total

        @pl.loop(0, n // 2)
        def _(k):
            target = 4 * far_first(k // 2, n // 4) + col * 2 + lax.rem(k, 2)

            @pl.when((target != me) & (target >= LEADS))
            def _():
                give(total_out, target, sum_group)

        cross.wait_send()

    for c in range(heads):
        with jax.named_scope(f"w_back{c}"):
            for d in range(2):
                each(d, True, lambda d=d, c=c: back(d, c).wait_recv())
        for t in range(2):
            for i in range(nb):
                total = rback[0, c, i, t].astype(F32) + rback[1, c, i, t].astype(F32)
                own[c, i, t] = own[c, i, t] + total

    flag = jnp.where(owner_ref[0] == me, 1.0, 0.0)
    hot_twice = (jnp.concatenate([hot, hot], axis=1).astype(F32) * flag).astype(BF16)

    for c in range(heads):
        for d in range(2):
            for t in range(2):
                each(d, False, lambda d=d, c=c, t=t: halo(d, c, t).wait_send())
            each(d, False, lambda d=d, c=c: back(d, c).wait_send())

    @pl.when(odd)
    def _():
        pass_on.wait_send()

    @pl.when(mine_hub)
    def _():
        drain(hub_in, n // 2 - 1, hs_sem.at[1])

    @pl.when(adder)
    def _():
        drain(hub2_in, n // 2 - 1, hs_sem.at[3])

    for extra_sends in (1, LEADS):
        @pl.when(adder & (col == 1) & ((other_sum < LEADS) == (extra_sends < LEADS)))
        def _():
            drain(hub2_in, extra_sends, hs_sem.at[3])

    drain_own(gsend, heads, hs_sem.at[0], mine_hub)
    drain_own(gpart, heads, hs_sem.at[2], adder)

    with jax.named_scope("w_gall2"):
        for is_adder_too in range(2):
            for leads in range(2):
                @pl.when((adder if is_adder_too else ~adder) & (lead if leads else ~lead))
                def _():
                    drain(sums, (heads - is_adder_too) * (1 + leads), hr_sem.at[3])

    for c in range(heads):
        for t, out in enumerate((dk_ref, dv_ref)):
            both = jnp.concatenate([sums[c, t], sums[heads + c, t]], axis=0)
            extra = nn(hot_twice, both)
            for i in range(nb):
                rsl = slice(i * BLOCK, (i + 1) * BLOCK)
                out[0, rsl, c * DH : (c + 1) * DH] = (own[c, i, t] + extra[rsl]).astype(BF16)


def write_out(*refs):
    copies = [
        pltpu.make_async_copy(refs[i], refs[3 + i], refs[6].at[i]) for i in range(3)
    ]
    for cp in copies:
        cp.start()
    for cp in copies:
        cp.wait()


def solution(mesh):
    n = mesh.shape["seq"]

    def local(query, keys, values, grad_out, global_offset, owner, block_lists):
        rows, qw = query.shape[1:]
        kw = keys.shape[2]
        heads = kw // DH
        group = HQ // HK
        nb = rows // BLOCK
        listed = block_lists.shape[2]
        gtok = global_offset.shape[1]
        hubs = 2 * heads
        wide = nb + 2 * REACH
        assert nb == REACH and n % 8 == 0 and n >= 2 * hubs and heads % 2 == 0
        vm = pl.BlockSpec(memory_space=pltpu.VMEM)
        hb = pl.BlockSpec(memory_space=pl.ANY)
        held = pl.pallas_call(
            functools.partial(kernel, n, heads, group, nb, listed, gtok),
            out_shape=tuple(pltpu.VMEM(a.shape, BF16) for a in (query, keys, values)),
            in_specs=[hb] * 7,
            out_specs=(vm, vm, vm),
            scratch_shapes=[
                pltpu.SMEM(owner.shape, jnp.int32),
                pltpu.SMEM(block_lists.shape, jnp.int32),
                pltpu.VMEM(global_offset.shape, jnp.int32),
                pltpu.SemaphoreType.DMA((3,)),
                pltpu.VMEM((rows, qw), BF16),
                pltpu.VMEM((rows, qw), BF16),
                pltpu.VMEM((heads, 2, gtok, DH), BF16),
                pltpu.VMEM((n // 2, 2, gtok, DH), BF16),
                pltpu.VMEM((2, gtok, DH), BF16),
                pltpu.VMEM((2 * heads, 2, gtok, DH), BF16),
                pltpu.VMEM((heads, 2, gtok, DH), BF16),
                pltpu.SemaphoreType.DMA((2,)),
                pltpu.VMEM((heads, 2, gtok, DH), BF16),
                pltpu.VMEM((n // 2, 2, gtok, DH), BF16),
                pltpu.VMEM((2, gtok, DH), BF16),
                pltpu.VMEM((2, gtok, DH), BF16),
                pltpu.VMEM((2, gtok, DH), BF16),
                pltpu.VMEM((2 * heads, 2, gtok, DH), BF16),
                pltpu.SemaphoreType.DMA((2,)),
                pltpu.VMEM((heads, nb, listed * BLOCK, group * BLOCK), F32),
                pltpu.VMEM((heads, nb, listed * BLOCK, group * BLOCK), F32),
                pltpu.VMEM((heads, nb, listed * BLOCK + gtok, group * BLOCK), BF16),
                pltpu.VMEM((nb, listed + 1, 2, BLOCK, DH), F32),
                pltpu.VMEM((heads, nb, 2, BLOCK, DH), F32),
                pltpu.VMEM((2, heads, REACH, 2, BLOCK, DH), BF16),
                pltpu.VMEM((2, heads, REACH, 2, BLOCK, DH), BF16),
                pltpu.SemaphoreType.DMA((2 * heads * nb,)),
                pltpu.SemaphoreType.DMA((2,)),
                pltpu.SemaphoreType.DMA((4 * heads,)),
                pltpu.SemaphoreType.DMA((4 * heads,)),
                pltpu.SemaphoreType.DMA((2 * heads,)),
                pltpu.SemaphoreType.DMA((2 * heads,)),
                pltpu.SemaphoreType.DMA((4,)),
                pltpu.SemaphoreType.DMA((4,)),
            ]
            + [pltpu.VMEM((wide, BLOCK, DH), BF16)] * (2 * heads),
            compiler_params=pltpu.CompilerParams(collective_id=0, has_side_effects=True),
        )(owner, block_lists, global_offset, query, keys, values, grad_out)
        return pl.pallas_call(
            write_out,
            out_shape=tuple(jax.ShapeDtypeStruct(a.shape, BF16) for a in (query, keys, values)),
            in_specs=[hb] * 3,
            out_specs=[hb] * 3,
            scratch_shapes=[pltpu.SemaphoreType.DMA((3,))],
        )(*[pltpu.with_memory_space_constraint(a, pltpu.VMEM) for a in held])

    return jax.shard_map(
        local,
        mesh=mesh,
        in_specs=(
            P(None, "seq", "head"),
            P(None, "seq", "head"),
            P(None, "seq", "head"),
            P(None, "seq", "head"),
            P(),
            P(),
            P(None, "seq", None),
        ),
        out_specs=(P(None, "seq", "head"), P(None, "seq", "head"), P(None, "seq", "head")),
        check_vma=False,
    )
```

```python
import functools

import jax
import jax.numpy as jnp
from jax import lax
from jax.experimental import pallas as pl
from jax.experimental.pallas import tpu as pltpu
from jax.sharding import PartitionSpec as P

HQ = 16
HK = 4
DH = 128
BLOCK = 128
REACH = 2
LEADS = 2
LOG2E = 1.4426950408889634
F32 = jnp.float32
BF16 = jnp.bfloat16


def nt(a, b):
    return lax.dot_general(a, b, (((1,), (1,)), ((), ())), preferred_element_type=F32)


def nn(a, b):
    return lax.dot_general(a, b, (((1,), (0,)), ((), ())), preferred_element_type=F32)


def kernel(
    n, heads, group, nb, listed, gtok,
    owner_hbm, lists_hbm, goff_hbm, q_hbm, k_hbm, v_hbm, g_hbm,
    dq_ref, own, sums_out, hot_out,
    owner_ref, lists_ref, goff_ref, small_sem, qv, gv, gsend, hub_in, hub_out, gcand, gall, fw_sem, gpart, hub2_in, half_out, total_out, cross_in, sums, sum_sem, cross_sem,
    keep_ex, keep_dp, keep_ds, wslot, sback, rback, load_sem, big_sem, ks_sem, kr_sem, gs_sem, gr_sem, hs_sem, hr_sem,
    *kvw,
):
    me = lax.axis_index("seq")
    hubs = 2 * heads
    rows = nb * BLOCK
    first = n // 2 - hubs + 1
    hub = (me - first) // 2
    col = lax.rem(me // 2, 2)
    lane = (me // 4) * 2 + lax.rem(me, 2)
    odd = lax.rem(me, 2) == 1
    level = hub // 2
    group_of = jnp.where(col == 0, level, heads - 1 - level)

    def row_of(g, side):
        return jnp.where(side == 0, g, heads - 1 - g)

    def hub_id(g, side):
        return first + 4 * row_of(g, side) + 2 * side

    def sum_id(t, side):
        return 4 * jnp.where(side == 0, 1 + t, 2 - t) + 2 * side + 1

    row = me // 4
    adder = odd & (row > 0) & (row < 3)
    sum_t = jnp.clip(jnp.where(col == 0, row - 1, 2 - row), 0, 1)
    other_sum = sum_id(sum_t, 1 - col)

    def hubbed(i):
        return (i >= first) & (i < first + 2 * hubs) & (lax.rem(i + first, 2) == 0)

    src_refs = (k_hbm, v_hbm)
    loads = []
    for t in range(2):
        for c in range(heads):
            for i in range(nb):
                cp = pltpu.make_async_copy(
                    src_refs[t].at[0, pl.ds(i * BLOCK, BLOCK), pl.ds(c * DH, DH)],
                    kvw[t * heads + c].at[REACH + i],
                    load_sem.at[(t * heads + c) * nb + i],
                )
                cp.start()
                loads.append(cp)
    small = [
        pltpu.make_async_copy(a, b, small_sem.at[i])
        for i, (a, b) in enumerate(
            ((goff_hbm, goff_ref), (owner_hbm, owner_ref), (lists_hbm, lists_ref))
        )
    ]
    for cp in small:
        cp.start()

    barrier = pltpu.get_barrier_semaphore()

    def greet(other):
        pl.semaphore_signal(
            barrier, inc=1, device_id={"seq": other}, device_id_type=pl.DeviceIdType.MESH
        )

    mine_hub = hubbed(me)

    @pl.when(mine_hub)
    def _():
        @pl.loop(0, n // 2)
        def _(k):
            target = (k // 2) * 4 + col * 2 + lax.rem(k, 2)

            @pl.when((target != me) & (target != me - 1))
            def _():
                greet(target)

    @pl.when(odd)
    def _():
        for g in range(heads):
            greet(hub_id(g, 1 - col))

    @pl.when(me > 0)
    def _():
        greet(me - 1)

    @pl.when(me < n - 1)
    def _():
        greet(me + 1)

    cq = pltpu.make_async_copy(q_hbm.at[0], qv, big_sem.at[0])
    cg = pltpu.make_async_copy(g_hbm.at[0], gv, big_sem.at[1])

    with jax.named_scope("w_loads"):
        small[0].wait()
        for cp in loads:
            cp.wait()
    cq.start()
    cg.start()

    hot = lax.broadcasted_iota(jnp.int32, (rows, gtok), 0) == goff_ref[...]
    hot = jnp.where(hot, 1.0, 0.0).astype(BF16)
    for t in range(2):
        for c in range(heads):
            mine = kvw[t * heads + c][REACH : REACH + nb].reshape(rows, DH)
            got = lax.dot_general(hot, mine, (((0,), (0,)), ((), ())), preferred_element_type=F32)
            gsend[c, t] = got.astype(BF16)
    zeros_kv = jnp.zeros((REACH, BLOCK, DH), BF16)

    @pl.when(me == 0)
    def _():
        for ref in kvw:
            ref[0:REACH] = zeros_kv
        rback[0] = jnp.zeros(rback.shape[1:], BF16)

    @pl.when(me == n - 1)
    def _():
        for ref in kvw:
            ref[REACH + nb : REACH + nb + REACH] = zeros_kv
        rback[1] = jnp.zeros(rback.shape[1:], BF16)

    lead = me < LEADS

    @pl.when(~lead)
    def _():
        sums[2 * heads :] = jnp.zeros((2 * heads, gtok, DH), BF16)

    zero_tile = jnp.zeros((nb, 2, BLOCK, DH), F32)
    wslot[:, listed] = zero_tile

    beside = jnp.where(me > 0, 1, 0) + jnp.where(me < n - 1, 1, 0)
    greeted = heads + jnp.where(mine_hub, n // 4 - 1, 0) - jnp.where(hubbed(me + 1), 1, 0)
    with jax.named_scope("w_barrier"):
        pl.semaphore_wait(barrier, beside + greeted)

    def remote(src, dst, s_sem, r_sem, target):
        return pltpu.make_async_remote_copy(
            src_ref=src, dst_ref=dst, send_sem=s_sem, recv_sem=r_sem,
            device_id={"seq": target}, device_id_type=pl.DeviceIdType.MESH,
        )

    def to_hub(src, dst, i, g, target):
        @pl.when(me != target)
        def _():
            remote(src.at[g], dst.at[lane], hs_sem.at[i], hr_sem.at[i], target).start()

    def drain(ref, count, sem):
        part = ref.at[pl.ds(0, count)]
        pltpu.make_async_copy(part, part, sem).wait()

    for g in range(heads):
        to_hub(gsend, hub_in, 0, g, hub_id(g, col))

    def halo(direction, c, t):
        idx = (direction * heads + c) * 2 + t
        ref = kvw[t * heads + c]
        if direction == 0:
            src, dst, target = ref.at[pl.ds(nb, REACH)], ref.at[pl.ds(0, REACH)], me + 1
        else:
            src, dst, target = ref.at[pl.ds(REACH, REACH)], ref.at[pl.ds(REACH + nb, REACH)], me - 1
        return remote(src, dst, ks_sem.at[idx], kr_sem.at[idx], target)

    def back(direction, c):
        idx = direction * heads + c
        target = me + 1 if direction == 0 else me - 1
        return remote(
            sback.at[direction, c], rback.at[direction, c], gs_sem.at[idx], gr_sem.at[idx], target
        )

    def each(direction, receiving, what):
        up = (direction == 0) != receiving
        cond = me < n - 1 if up else me > 0
        pl.when(cond)(what)

    place = lax.rem(me, 4)

    def far(d):
        return place == (3 if d == 0 else 0)

    def halo_start(c, d, late):
        for t in range(2):
            cond = (me < n - 1 if d == 0 else me > 0) & (far(d) if late else ~far(d))
            pl.when(cond)(lambda t=t: halo(d, c, t).start())

    held = mine_hub & (place == 1)

    halo_start(0, 0, False)
    halo_start(0, 1, False)
    for c in range(1, heads):
        halo_start(c, 1, False)
        pl.when(~held)(functools.partial(halo_start, c, 0, False))
    for c in range(heads):
        for d in range(2):
            halo_start(c, d, True)

    def halo_wait(c, paired):
        for d in range(2):
            cond = (me > 0 if d == 0 else me < n - 1) & ((odd if d == 0 else ~odd) == paired)
            for t in range(2):
                pl.when(cond)(lambda d=d, t=t: halo(d, c, t).wait_recv())

    for cp in small[1:]:
        cp.wait()

    with jax.named_scope('w_qg'):
        cq.wait()
        cg.wait()
    scale = DH ** (-0.5)
    fold = scale * LOG2E
    local_idx = [
        [
            jnp.clip(lists_ref[0, b, l] - me * nb + REACH, 0, nb + 2 * REACH - 1)
            for l in range(listed)
        ]
        for b in range(nb)
    ]

    def near_rows(t, c, b):
        return [kvw[t * heads + c][local_idx[b][l]] for l in range(1, listed)]

    def columns(c):
        return [slice((c * group + i) * DH, (c * group + i + 1) * DH) for i in range(group)]

    def stacked(ref, c, b):
        rsl = slice(b * BLOCK, (b + 1) * BLOCK)
        return jnp.concatenate([ref[rsl, s] for s in columns(c)], axis=0)

    def logits(ks, vs, c, b):
        return nt(ks, stacked(qv, c, b)), nt(vs, stacked(gv, c, b))

    def keep(c, b, start, st, dp):
        top = jnp.max(st, axis=0, keepdims=True)
        ex = jnp.exp2((st - top) * fold)
        keep_ex[c, b, start : start + st.shape[0]] = ex
        keep_dp[c, b, start : start + st.shape[0]] = dp
        total = jnp.sum(ex, axis=0, keepdims=True)
        return top, total, jnp.sum(ex * dp, axis=0, keepdims=True)

    window = listed * BLOCK
    stats = {}
    for c in range(heads):
        for b in range(nb):
            kb, vb = kvw[c][REACH + b], kvw[heads + c][REACH + b]
            stats[c, b] = [keep(c, b, 0, *logits(kb, vb, c, b))]

    def far_first(i, count):
        return jnp.where(lax.rem(i, 2) == 0, count - 1 - i // 2, i // 2)

    owner_at = owner_ref[0]

    @pl.when(mine_hub)
    def _():
        with jax.named_scope("w_hub1"):
            drain(hub_in, n // 2 - 1, hr_sem.at[0])
        hub_in[lane] = gsend[group_of]
        pick = hub_in[(owner_at // 4) * 2 + lax.rem(owner_at, 2)]
        hub_out[...] = pick
        gcand[col * heads + group_of] = pick

        @pl.loop(0, n // 2)
        def _(k):
            target = 4 * far_first(k // 2, n // 4) + 2 * lax.rem(k, 2) + 1

            @pl.when(target != me)
            def _():
                remote(
                    hub_out, gcand.at[col * heads + group_of], hs_sem.at[1], hr_sem.at[1], target
                ).start()

        @pl.when(held)
        def _():
            for c in range(1, heads):
                halo_start(c, 0, False)

    held_back = adder & (place == 3) & (other_sum > me)

    def back_start(c):
        for d in range(2):
            if c == heads - 1 and d == 0:
                ready = (me < n - 1) & ~held_back
                pl.when(ready)(lambda d=d: back(d, c).start())
            else:
                each(d, False, lambda d=d: back(d, c).start())

    def drain_own(ref, count, sem, self_served):
        @pl.when(self_served)
        def _():
            drain(ref, count - 1, sem)

        @pl.when(~self_served)
        def _():
            drain(ref, count, sem)

    pass_on = remote(gall, gall, fw_sem.at[0], fw_sem.at[1], jnp.where(odd, me - 1, me + 1))

    def collect():
        with jax.named_scope("w_cand"):
            drain_own(gcand, 2 * heads, hr_sem.at[1], mine_hub)
        side = lax.rem(owner_at // 2, 2) * heads
        for g in range(heads):
            gall[g] = gcand[side + g]
        pass_on.start()

    ratios = {}
    for c in range(heads):
        last = c == heads - 1
        with jax.named_scope(f"w_halo{c}"):
            halo_wait(c, True)
            halo_wait(c, False)
        if not last:
            for b in range(nb):
                kn = jnp.concatenate(near_rows(0, c, b), axis=0)
                vn = jnp.concatenate(near_rows(1, c, b), axis=0)
                stats[c, b].append(keep(c, b, BLOCK, *logits(kn, vn, c, b)))
        if c == 0:
            pl.when(odd)(collect)
            with jax.named_scope("w_gall"):
                @pl.when(~odd)
                def _():
                    pass_on.wait_recv()
        glob = [None, None]
        for b in range(nb):
            qs, gs = stacked(qv, c, b), stacked(gv, c, b)
            kn, vn = [gall[c, 0]], [gall[c, 1]]
            if last:
                kn, vn = near_rows(0, c, b) + kn, near_rows(1, c, b) + vn
            st, dp = logits(jnp.concatenate(kn, axis=0), jnp.concatenate(vn, axis=0), c, b)
            top = jnp.max(st, axis=0, keepdims=True)
            for old in stats[c, b]:
                top = jnp.maximum(top, old[0])
            ex = jnp.exp2((st - top) * fold)
            total = jnp.sum(ex, axis=0, keepdims=True)
            dot = jnp.sum(ex * dp, axis=0, keepdims=True)
            shrinks = [jnp.exp2((old[0] - top) * fold) for old in stats[c, b]]
            for shrink, old in zip(shrinks, stats[c, b]):
                total = total + old[1] * shrink
                dot = dot + old[2] * shrink
            inv = 1.0 / total
            dot = dot * inv
            if last:
                near = window - BLOCK
                keep_ex[c, b, BLOCK:window] = ex[:near]
                keep_dp[c, b, BLOCK:window] = dp[:near]
                ex, dp = ex[near:], dp[near:]
            pr = ex * inv
            ds = (pr * (dp - dot)).astype(BF16)
            keep_ds[c, b, window:] = ds
            own_ratio = shrinks[0] * inv
            ratios[c, b] = (own_ratio, inv if last else shrinks[1] * inv, dot)
            for t, part in enumerate((nn(ds, qs) * scale, nn(pr.astype(BF16), gs))):
                glob[t] = part if glob[t] is None else glob[t] + part
        for t in range(2):
            gpart[2 * c + t] = glob[t].astype(BF16)
        with jax.named_scope(f"s_gpart{c}"):
            for t in range(2):
                target = sum_id(t, col)

                @pl.when(me != target)
                def _():
                    remote(
                        gpart.at[2 * c + t], hub2_in.at[c, lane], hs_sem.at[2], sum_sem.at[c], target
                    ).start()

    for c in range(heads):
        for b in range(nb):
            qs, gs = stacked(qv, c, b), stacked(gv, c, b)
            own_ratio, near_ratio, dot = ratios[c, b]
            vals = []
            for lo, hi, ratio in ((0, BLOCK, own_ratio), (BLOCK, window, near_ratio)):
                pr = keep_ex[c, b, lo:hi] * ratio
                ds = (pr * (keep_dp[c, b, lo:hi] - dot)).astype(BF16)
                keep_ds[c, b, lo:hi] = ds
                vals.append((ds, pr.astype(BF16)))
            ds, pr = (jnp.concatenate([v[i] for v in vals], axis=0) for i in range(2))
            for t, val in enumerate((nn(ds, qs) * scale, nn(pr, gs))):
                for l in range(listed):
                    wslot[b, l, t] = val[l * BLOCK : (l + 1) * BLOCK]
        for dst in range(nb + 2 * REACH):
            total = None
            for b in range(nb):
                if not b <= dst <= b + 2 * REACH:
                    continue
                slot = jnp.int32(listed)
                for l in range(1, listed):
                    slot = jnp.where(local_idx[b][l] == dst, l, slot)
                term = wslot[b, 0] if dst == b + REACH else wslot[b, slot]
                total = term if total is None else total + term
            if dst < REACH:
                sback[1, c, dst] = total.astype(BF16)
            elif dst < REACH + nb:
                own[c, dst - REACH] = total
            else:
                sback[0, c, dst - REACH - nb] = total.astype(BF16)
        with jax.named_scope(f"s_back{c}"):
            back_start(c)

    for c in range(heads):
        for b in range(nb):
            ks = jnp.concatenate([kvw[c][REACH + b]] + near_rows(0, c, b) + [gall[c, 0]], axis=0)
            dqt = nn(ks.T, keep_ds[c, b]) * scale
            dq = dqt.T.astype(BF16)
            for i, s in enumerate(columns(c)):
                dq_ref[0, b * BLOCK : (b + 1) * BLOCK, s] = dq[i * BLOCK : (i + 1) * BLOCK]

    def give(src, target, at):
        remote(src, sums.at[at], hs_sem.at[3], hr_sem.at[3], target).start()

    def cross(c):
        return remote(
            half_out.at[c], cross_in.at[c], cross_sem.at[c], cross_sem.at[heads + c], other_sum
        )

    @pl.when(adder)
    def _():
        halves = []
        for c in range(heads):
            with jax.named_scope(f"w_hub2{c}"):
                drain(hub2_in.at[c], n // 2 - 1, sum_sem.at[c])
            hub2_in[c, lane] = gpart[2 * c + sum_t]
            half = jnp.sum(hub2_in[c].astype(F32), axis=0)
            halves.append(half)
            half_out[c] = half.astype(BF16)
            cross(c).start()
            for target in range(LEADS):
                give(half_out.at[c], target, 2 * (col * heads + c) + sum_t)

        @pl.when(held_back)
        def _():
            back(0, heads - 1).start()

        for c in range(heads):
            with jax.named_scope(f"w_cross{c}"):
                cross(c).wait_recv()
            total = (halves[c] + cross_in[c].astype(F32)).astype(BF16)
            total_out[c] = total
            sums[2 * c + sum_t] = total

            @pl.loop(0, n // 2)
            def _(k):
                target = 4 * far_first(k // 2, n // 4) + col * 2 + lax.rem(k, 2)

                @pl.when((target != me) & (target >= LEADS))
                def _():
                    give(total_out.at[c], target, 2 * c + sum_t)

    for c in range(heads):
        with jax.named_scope(f"w_back{c}"):
            for d in range(2):
                each(d, True, lambda d=d, c=c: back(d, c).wait_recv())
        for t in range(2):
            for i in range(nb):
                total = rback[0, c, i, t].astype(F32) + rback[1, c, i, t].astype(F32)
                own[c, i, t] = own[c, i, t] + total

    flag = jnp.where(owner_ref[0] == me, 1.0, 0.0)
    hot_out[...] = (jnp.concatenate([hot, hot], axis=1).astype(F32) * flag).astype(BF16)

    for c in range(heads):
        for d in range(2):
            for t in range(2):
                each(d, False, lambda d=d, c=c, t=t: halo(d, c, t).wait_send())
            each(d, False, lambda d=d, c=c: back(d, c).wait_send())

    @pl.when(odd)
    def _():
        pass_on.wait_send()

    @pl.when(mine_hub)
    def _():
        drain(hub_in, n // 2 - 1, hs_sem.at[1])

    @pl.when(adder)
    def _():
        for c in range(heads):
            drain(hub2_in.at[c], n // 2 - 1, hs_sem.at[3])
            cross(c).wait_send()

    @pl.when(adder & (col == 1))
    def _():
        drain(gpart, LEADS * heads, hs_sem.at[3])

    drain_own(gsend, heads, hs_sem.at[0], mine_hub)
    for self_served in range(2):
        @pl.when(adder if self_served else ~adder)
        def _():
            drain(gpart, heads * (2 - self_served), hs_sem.at[2])


    with jax.named_scope("w_gall2"):
        for who, count in ((lead, 4), (adder, 1), (~lead & ~adder, 2)):
            @pl.when(who)
            def _():
                drain(sums, count * heads, hr_sem.at[3])

    sums_out[...] = sums[...]


def write_out(heads, dq_ref, own, sums, hot, dq_out, dk_out, dv_out, dk_ref, dv_ref, sem):
    first = pltpu.make_async_copy(dq_ref, dq_out, sem.at[0])
    first.start()
    copies = [first]
    for t, (held, out) in enumerate(((dk_ref, dk_out), (dv_ref, dv_out))):
        for c in range(heads):
            both = jnp.concatenate([sums[2 * c + t], sums[2 * (heads + c) + t]], axis=0)
            extra = nn(hot[...], both)
            for i in range(own.shape[1]):
                rsl = slice(i * BLOCK, (i + 1) * BLOCK)
                held[0, rsl, c * DH : (c + 1) * DH] = (own[c, i, t] + extra[rsl]).astype(BF16)
        cp = pltpu.make_async_copy(held, out, sem.at[1 + t])
        cp.start()
        copies.append(cp)
    for cp in copies:
        cp.wait()


def solution(mesh):
    n = mesh.shape["seq"]

    def local(query, keys, values, grad_out, global_offset, owner, block_lists):
        rows, qw = query.shape[1:]
        kw = keys.shape[2]
        heads = kw // DH
        group = HQ // HK
        nb = rows // BLOCK
        listed = block_lists.shape[2]
        gtok = global_offset.shape[1]
        hubs = 2 * heads
        wide = nb + 2 * REACH
        assert nb == REACH and n % 8 == 0 and n >= 2 * hubs and heads % 2 == 0
        vm = pl.BlockSpec(memory_space=pltpu.VMEM)
        hb = pl.BlockSpec(memory_space=pl.ANY)
        held = pl.pallas_call(
            functools.partial(kernel, n, heads, group, nb, listed, gtok),
            out_shape=(
                pltpu.VMEM(query.shape, BF16),
                pltpu.VMEM((heads, nb, 2, BLOCK, DH), F32),
                pltpu.VMEM((4 * heads, gtok, DH), BF16),
                pltpu.VMEM((rows, 2 * gtok), BF16),
            ),
            in_specs=[hb] * 7,
            out_specs=(vm,) * 4,
            scratch_shapes=[
                pltpu.SMEM(owner.shape, jnp.int32),
                pltpu.SMEM(block_lists.shape, jnp.int32),
                pltpu.VMEM(global_offset.shape, jnp.int32),
                pltpu.SemaphoreType.DMA((3,)),
                pltpu.VMEM((rows, qw), BF16),
                pltpu.VMEM((rows, qw), BF16),
                pltpu.VMEM((heads, 2, gtok, DH), BF16),
                pltpu.VMEM((n // 2, 2, gtok, DH), BF16),
                pltpu.VMEM((2, gtok, DH), BF16),
                pltpu.VMEM((2 * heads, 2, gtok, DH), BF16),
                pltpu.VMEM((heads, 2, gtok, DH), BF16),
                pltpu.SemaphoreType.DMA((2,)),
                pltpu.VMEM((2 * heads, gtok, DH), BF16),
                pltpu.VMEM((heads, n // 2, gtok, DH), BF16),
                pltpu.VMEM((heads, gtok, DH), BF16),
                pltpu.VMEM((heads, gtok, DH), BF16),
                pltpu.VMEM((heads, gtok, DH), BF16),
                pltpu.VMEM((4 * heads, gtok, DH), BF16),
                pltpu.SemaphoreType.DMA((heads,)),
                pltpu.SemaphoreType.DMA((2 * heads,)),
                pltpu.VMEM((heads, nb, listed * BLOCK, group * BLOCK), F32),
                pltpu.VMEM((heads, nb, listed * BLOCK, group * BLOCK), F32),
                pltpu.VMEM((heads, nb, listed * BLOCK + gtok, group * BLOCK), BF16),
                pltpu.VMEM((nb, listed + 1, 2, BLOCK, DH), F32),
                pltpu.VMEM((2, heads, REACH, 2, BLOCK, DH), BF16),
                pltpu.VMEM((2, heads, REACH, 2, BLOCK, DH), BF16),
                pltpu.SemaphoreType.DMA((2 * heads * nb,)),
                pltpu.SemaphoreType.DMA((2,)),
                pltpu.SemaphoreType.DMA((4 * heads,)),
                pltpu.SemaphoreType.DMA((4 * heads,)),
                pltpu.SemaphoreType.DMA((2 * heads,)),
                pltpu.SemaphoreType.DMA((2 * heads,)),
                pltpu.SemaphoreType.DMA((4,)),
                pltpu.SemaphoreType.DMA((4,)),
            ]
            + [pltpu.VMEM((wide, BLOCK, DH), BF16)] * (2 * heads),
            compiler_params=pltpu.CompilerParams(collective_id=0, has_side_effects=True),
        )(owner, block_lists, global_offset, query, keys, values, grad_out)
        return pl.pallas_call(
            functools.partial(write_out, heads),
            out_shape=tuple(jax.ShapeDtypeStruct(a.shape, BF16) for a in (query, keys, values)),
            in_specs=[hb, vm, vm, vm],
            out_specs=[hb] * 3,
            scratch_shapes=[
                pltpu.VMEM(keys.shape, BF16),
                pltpu.VMEM(values.shape, BF16),
                pltpu.SemaphoreType.DMA((3,)),
            ],
        )(*[pltpu.with_memory_space_constraint(a, pltpu.VMEM) for a in held])

    return jax.shard_map(
        local,
        mesh=mesh,
        in_specs=(
            P(None, "seq", "head"),
            P(None, "seq", "head"),
            P(None, "seq", "head"),
            P(None, "seq", "head"),
            P(),
            P(),
            P(None, "seq", None),
        ),
        out_specs=(P(None, "seq", "head"), P(None, "seq", "head"), P(None, "seq", "head")),
        check_vma=False,
    )
```

```python
import functools

import jax
import jax.numpy as jnp
from jax import lax
from jax.experimental import pallas as pl
from jax.experimental.pallas import tpu as pltpu
from jax.sharding import PartitionSpec as P

HQ = 16
HK = 4
DH = 128
BLOCK = 128
REACH = 2
LEADS = 2
LOG2E = 1.4426950408889634
F32 = jnp.float32
BF16 = jnp.bfloat16


def nt(a, b):
    return lax.dot_general(a, b, (((1,), (1,)), ((), ())), preferred_element_type=F32)


def nn(a, b):
    return lax.dot_general(a, b, (((1,), (0,)), ((), ())), preferred_element_type=F32)


def kernel(
    n, heads, group, nb, listed, gtok,
    owner_hbm, lists_hbm, goff_hbm, q_hbm, k_hbm, v_hbm, g_hbm,
    dq_ref, own, sums_out, hot_out,
    owner_ref, lists_ref, goff_ref, small_sem, qv, gv, gsend, hub_in, hub_out, cand_sem, gall, fw_sem, gpart, hub2_in, half_out, total_out, cross_in, sums, sum_sem, cross_sem,
    keep_ex, keep_dp, keep_ds, wslot, sback, rback, load_sem, big_sem, ks_sem, kr_sem, gs_sem, gr_sem, hs_sem, hr_sem,
    *rest,
):
    kvw, gcand = rest[: 2 * heads], rest[2 * heads :]
    me = lax.axis_index("seq")
    hubs = 2 * heads
    rows = nb * BLOCK
    first = n // 2 - hubs + 1
    hub = (me - first) // 2
    col = lax.rem(me // 2, 2)
    lane = (me // 4) * 2 + lax.rem(me, 2)
    odd = lax.rem(me, 2) == 1
    level = hub // 2
    group_of = jnp.where(col == 0, level, heads - 1 - level)

    def row_of(g, side):
        return jnp.where(side == 0, g, heads - 1 - g)

    def hub_id(g, side):
        return first + 4 * row_of(g, side) + 2 * side

    def sum_id(t, side):
        return 4 * jnp.where(side == 0, 1 + t, 2 - t) + 2 * side + 1

    row = me // 4
    adder = odd & (row > 0) & (row < 3)
    sum_t = jnp.clip(jnp.where(col == 0, row - 1, 2 - row), 0, 1)
    other_sum = sum_id(sum_t, 1 - col)

    def hubbed(i):
        return (i >= first) & (i < first + 2 * hubs) & (lax.rem(i + first, 2) == 0)

    src_refs = (k_hbm, v_hbm)
    loads = []
    for t in range(2):
        for c in range(heads):
            for i in range(nb):
                cp = pltpu.make_async_copy(
                    src_refs[t].at[0, pl.ds(i * BLOCK, BLOCK), pl.ds(c * DH, DH)],
                    kvw[t * heads + c].at[REACH + i],
                    load_sem.at[(t * heads + c) * nb + i],
                )
                cp.start()
                loads.append(cp)
    small = [
        pltpu.make_async_copy(a, b, small_sem.at[i])
        for i, (a, b) in enumerate(
            ((goff_hbm, goff_ref), (owner_hbm, owner_ref), (lists_hbm, lists_ref))
        )
    ]
    for cp in small:
        cp.start()

    barrier = pltpu.get_barrier_semaphore()

    def greet(other):
        pl.semaphore_signal(
            barrier, inc=1, device_id={"seq": other}, device_id_type=pl.DeviceIdType.MESH
        )

    mine_hub = hubbed(me)

    @pl.when(mine_hub)
    def _():
        @pl.loop(0, n // 2)
        def _(k):
            target = (k // 2) * 4 + col * 2 + lax.rem(k, 2)

            @pl.when((target != me) & (target != me - 1))
            def _():
                greet(target)

    @pl.when(odd)
    def _():
        for g in range(heads):
            greet(hub_id(g, 1 - col))

    @pl.when(me > 0)
    def _():
        greet(me - 1)

    @pl.when(me < n - 1)
    def _():
        greet(me + 1)

    cq = pltpu.make_async_copy(q_hbm.at[0], qv, big_sem.at[0])
    cg = pltpu.make_async_copy(g_hbm.at[0], gv, big_sem.at[1])

    with jax.named_scope("w_loads"):
        small[0].wait()
        for cp in loads:
            cp.wait()
    cq.start()
    cg.start()

    hot = lax.broadcasted_iota(jnp.int32, (rows, gtok), 0) == goff_ref[...]
    hot = jnp.where(hot, 1.0, 0.0).astype(BF16)
    for t in range(2):
        for c in range(heads):
            mine = kvw[t * heads + c][REACH : REACH + nb].reshape(rows, DH)
            got = lax.dot_general(hot, mine, (((0,), (0,)), ((), ())), preferred_element_type=F32)
            gsend[t, c] = got.astype(BF16)
    zeros_kv = jnp.zeros((REACH, BLOCK, DH), BF16)

    @pl.when(me == 0)
    def _():
        for ref in kvw:
            ref[0:REACH] = zeros_kv
        rback[0] = jnp.zeros(rback.shape[1:], BF16)

    @pl.when(me == n - 1)
    def _():
        for ref in kvw:
            ref[REACH + nb : REACH + nb + REACH] = zeros_kv
        rback[1] = jnp.zeros(rback.shape[1:], BF16)

    lead = me < LEADS

    @pl.when(~lead)
    def _():
        sums[2 * heads :] = jnp.zeros((2 * heads, gtok, DH), BF16)

    zero_tile = jnp.zeros((nb, 2, BLOCK, DH), F32)
    wslot[:, listed] = zero_tile

    beside = jnp.where(me > 0, 1, 0) + jnp.where(me < n - 1, 1, 0)
    greeted = heads + jnp.where(mine_hub, n // 4 - 1, 0) - jnp.where(hubbed(me + 1), 1, 0)
    with jax.named_scope("w_barrier"):
        pl.semaphore_wait(barrier, beside + greeted)

    def remote(src, dst, s_sem, r_sem, target):
        return pltpu.make_async_remote_copy(
            src_ref=src, dst_ref=dst, send_sem=s_sem, recv_sem=r_sem,
            device_id={"seq": target}, device_id_type=pl.DeviceIdType.MESH,
        )

    def to_hub(src, dst, i, g, target):
        @pl.when(me != target)
        def _():
            remote(src.at[g], dst.at[lane], hs_sem.at[i], hr_sem.at[i], target).start()

    def drain(ref, count, sem):
        part = ref.at[pl.ds(0, count)]
        pltpu.make_async_copy(part, part, sem).wait()

    for g in range(heads):
        to_hub(gsend, hub_in, 0, g, hub_id(g, col))

    def halo(direction, c, t):
        idx = (direction * heads + c) * 2 + t
        ref = kvw[t * heads + c]
        if direction == 0:
            src, dst, target = ref.at[pl.ds(nb, REACH)], ref.at[pl.ds(0, REACH)], me + 1
        else:
            src, dst, target = ref.at[pl.ds(REACH, REACH)], ref.at[pl.ds(REACH + nb, REACH)], me - 1
        return remote(src, dst, ks_sem.at[idx], kr_sem.at[idx], target)

    def back(direction, c):
        idx = direction * heads + c
        target = me + 1 if direction == 0 else me - 1
        return remote(
            sback.at[direction, c], rback.at[direction, c], gs_sem.at[idx], gr_sem.at[idx], target
        )

    def each(direction, receiving, what):
        up = (direction == 0) != receiving
        cond = me < n - 1 if up else me > 0
        pl.when(cond)(what)

    place = lax.rem(me, 4)

    def far(d):
        return place == (3 if d == 0 else 0)

    def halo_start(c, d, late):
        for t in range(2):
            cond = (me < n - 1 if d == 0 else me > 0) & (far(d) if late else ~far(d))
            pl.when(cond)(lambda t=t: halo(d, c, t).start())

    held = mine_hub & (place == 1)

    halo_start(0, 0, False)
    halo_start(0, 1, False)
    for c in range(1, heads):
        halo_start(c, 1, False)
        pl.when(~held)(functools.partial(halo_start, c, 0, False))
    for c in range(heads):
        for d in range(2):
            halo_start(c, d, True)

    def halo_wait(c, paired):
        for d in range(2):
            cond = (me > 0 if d == 0 else me < n - 1) & ((odd if d == 0 else ~odd) == paired)
            for t in range(2):
                pl.when(cond)(lambda d=d, t=t: halo(d, c, t).wait_recv())

    for cp in small[1:]:
        cp.wait()

    with jax.named_scope('w_qg'):
        cq.wait()
        cg.wait()
    scale = DH ** (-0.5)
    fold = scale * LOG2E
    local_idx = [
        [
            jnp.clip(lists_ref[0, b, l] - me * nb + REACH, 0, nb + 2 * REACH - 1)
            for l in range(listed)
        ]
        for b in range(nb)
    ]

    def near_rows(t, c, b):
        return [kvw[t * heads + c][local_idx[b][l]] for l in range(1, listed)]

    def columns(c):
        return [slice((c * group + i) * DH, (c * group + i + 1) * DH) for i in range(group)]

    def stacked(ref, c, b):
        rsl = slice(b * BLOCK, (b + 1) * BLOCK)
        return jnp.concatenate([ref[rsl, s] for s in columns(c)], axis=0)

    def logits(ks, vs, c, b):
        return nt(ks, stacked(qv, c, b)), nt(vs, stacked(gv, c, b))

    def keep(c, b, start, st, dp):
        top = jnp.max(st, axis=0, keepdims=True)
        ex = jnp.exp2((st - top) * fold)
        keep_ex[c, b, start : start + st.shape[0]] = ex
        keep_dp[c, b, start : start + st.shape[0]] = dp
        total = jnp.sum(ex, axis=0, keepdims=True)
        return top, total, jnp.sum(ex * dp, axis=0, keepdims=True)

    window = listed * BLOCK
    stats = {}
    for c in range(heads):
        for b in range(nb):
            kb, vb = kvw[c][REACH + b], kvw[heads + c][REACH + b]
            stats[c, b] = [keep(c, b, 0, *logits(kb, vb, c, b))]

    def far_first(i, count):
        return jnp.where(lax.rem(i, 2) == 0, count - 1 - i // 2, i // 2)

    owner_at = owner_ref[0]

    @pl.when(mine_hub)
    def _():
        with jax.named_scope("w_hub1"):
            drain(hub_in, n // 2 - 1, hr_sem.at[0])
        hub_in[lane] = gsend[group_of]
        pick = hub_in[(owner_at // 4) * 2 + lax.rem(owner_at, 2)]
        hub_out[...] = pick
        for c in range(heads):
            gcand[c][2 * col + group_of] = pick[c]
        for c in range(heads):
            @pl.loop(0, n // 2)
            def _(k):
                target = 4 * far_first(k // 2, n // 4) + 2 * lax.rem(k, 2) + 1

                @pl.when(target != me)
                def _():
                    remote(
                        hub_out.at[c], gcand[c].at[2 * col + group_of],
                        hs_sem.at[1], cand_sem.at[c], target,
                    ).start()

        @pl.when(held)
        def _():
            for c in range(1, heads):
                halo_start(c, 0, False)

    held_back = adder & (place == 3) & (other_sum > me)

    def back_start(c):
        for d in range(2):
            if c == heads - 1 and d == 0:
                ready = (me < n - 1) & ~held_back
                pl.when(ready)(lambda d=d: back(d, c).start())
            else:
                each(d, False, lambda d=d: back(d, c).start())

    def drain_own(ref, count, sem, self_served):
        @pl.when(self_served)
        def _():
            drain(ref, count - 1, sem)

        @pl.when(~self_served)
        def _():
            drain(ref, count, sem)

    def pass_on(c):
        return remote(
            gall.at[c], gall.at[c], fw_sem.at[c], fw_sem.at[heads + c],
            jnp.where(odd, me - 1, me + 1),
        )

    def collect():
        side = lax.rem(owner_at // 2, 2) * 2
        for c in range(heads):
            with jax.named_scope(f"w_cand{c}"):
                drain_own(gcand[c], 4, cand_sem.at[c], mine_hub)
            for t in range(2):
                gall[c, t] = gcand[c][side + t]
            pass_on(c).start()

    ratios = {}

    def key_value_grads(c):
        for b in range(nb):
            qs, gs = stacked(qv, c, b), stacked(gv, c, b)
            own_ratio, near_ratio, dot = ratios[c, b]
            vals = []
            for lo, hi, ratio in ((0, BLOCK, own_ratio), (BLOCK, window, near_ratio)):
                pr = keep_ex[c, b, lo:hi] * ratio
                ds = (pr * (keep_dp[c, b, lo:hi] - dot)).astype(BF16)
                keep_ds[c, b, lo:hi] = ds
                vals.append((ds, pr.astype(BF16)))
            ds, pr = (jnp.concatenate([v[i] for v in vals], axis=0) for i in range(2))
            for t, val in enumerate((nn(ds, qs) * scale, nn(pr, gs))):
                for l in range(listed):
                    wslot[b, l, t] = val[l * BLOCK : (l + 1) * BLOCK]
        for dst in range(nb + 2 * REACH):
            total = None
            for b in range(nb):
                if not b <= dst <= b + 2 * REACH:
                    continue
                slot = jnp.int32(listed)
                for l in range(1, listed):
                    slot = jnp.where(local_idx[b][l] == dst, l, slot)
                term = wslot[b, 0] if dst == b + REACH else wslot[b, slot]
                total = term if total is None else total + term
            if dst < REACH:
                sback[1, c, dst] = total.astype(BF16)
            elif dst < REACH + nb:
                own[c, dst - REACH] = total
            else:
                sback[0, c, dst - REACH - nb] = total.astype(BF16)
        with jax.named_scope(f"s_back{c}"):
            back_start(c)

    for c in range(heads):
        last = c == heads - 1
        with jax.named_scope(f"w_halo{c}"):
            halo_wait(c, True)
            halo_wait(c, False)
        if not last:
            for b in range(nb):
                kn = jnp.concatenate(near_rows(0, c, b), axis=0)
                vn = jnp.concatenate(near_rows(1, c, b), axis=0)
                stats[c, b].append(keep(c, b, BLOCK, *logits(kn, vn, c, b)))
        if c == 0:
            pl.when(odd)(collect)
        with jax.named_scope(f"w_gall{c}"):
            @pl.when(~odd)
            def _():
                pass_on(c).wait_recv()
        glob = [None, None]
        for b in range(nb):
            qs, gs = stacked(qv, c, b), stacked(gv, c, b)
            kn, vn = [gall[c, 0]], [gall[c, 1]]
            if last:
                kn, vn = near_rows(0, c, b) + kn, near_rows(1, c, b) + vn
            st, dp = logits(jnp.concatenate(kn, axis=0), jnp.concatenate(vn, axis=0), c, b)
            top = jnp.max(st, axis=0, keepdims=True)
            for old in stats[c, b]:
                top = jnp.maximum(top, old[0])
            ex = jnp.exp2((st - top) * fold)
            total = jnp.sum(ex, axis=0, keepdims=True)
            dot = jnp.sum(ex * dp, axis=0, keepdims=True)
            shrinks = [jnp.exp2((old[0] - top) * fold) for old in stats[c, b]]
            for shrink, old in zip(shrinks, stats[c, b]):
                total = total + old[1] * shrink
                dot = dot + old[2] * shrink
            inv = 1.0 / total
            dot = dot * inv
            if last:
                near = window - BLOCK
                keep_ex[c, b, BLOCK:window] = ex[:near]
                keep_dp[c, b, BLOCK:window] = dp[:near]
                ex, dp = ex[near:], dp[near:]
            pr = ex * inv
            ds = (pr * (dp - dot)).astype(BF16)
            keep_ds[c, b, window:] = ds
            own_ratio = shrinks[0] * inv
            ratios[c, b] = (own_ratio, inv if last else shrinks[1] * inv, dot)
            for t, part in enumerate((nn(ds, qs) * scale, nn(pr.astype(BF16), gs))):
                glob[t] = part if glob[t] is None else glob[t] + part
        for t in range(2):
            gpart[2 * c + t] = glob[t].astype(BF16)
        with jax.named_scope(f"s_gpart{c}"):
            for t in range(2):
                target = sum_id(t, col)

                @pl.when(me != target)
                def _():
                    remote(
                        gpart.at[2 * c + t], hub2_in.at[c, lane], hs_sem.at[2], sum_sem.at[c], target
                    ).start()
        if c == 0:
            pl.when(odd)(functools.partial(key_value_grads, 0))

    pl.when(~odd)(functools.partial(key_value_grads, 0))
    for c in range(1, heads):
        key_value_grads(c)

    for c in range(heads):
        for b in range(nb):
            ks = jnp.concatenate([kvw[c][REACH + b]] + near_rows(0, c, b) + [gall[c, 0]], axis=0)
            dqt = nn(ks.T, keep_ds[c, b]) * scale
            dq = dqt.T.astype(BF16)
            for i, s in enumerate(columns(c)):
                dq_ref[0, b * BLOCK : (b + 1) * BLOCK, s] = dq[i * BLOCK : (i + 1) * BLOCK]

    def give(src, target, at):
        remote(src, sums.at[at], hs_sem.at[3], hr_sem.at[3], target).start()

    def cross(c):
        return remote(
            half_out.at[c], cross_in.at[c], cross_sem.at[c], cross_sem.at[heads + c], other_sum
        )

    @pl.when(adder)
    def _():
        halves = []
        for c in range(heads):
            with jax.named_scope(f"w_hub2{c}"):
                drain(hub2_in.at[c], n // 2 - 1, sum_sem.at[c])
            hub2_in[c, lane] = gpart[2 * c + sum_t]
            half = jnp.sum(hub2_in[c].astype(F32), axis=0)
            halves.append(half)
            half_out[c] = half.astype(BF16)
            cross(c).start()
            for target in range(LEADS):
                give(half_out.at[c], target, 2 * (col * heads + c) + sum_t)

        @pl.when(held_back)
        def _():
            back(0, heads - 1).start()

        for c in range(heads):
            with jax.named_scope(f"w_cross{c}"):
                cross(c).wait_recv()
            total = (halves[c] + cross_in[c].astype(F32)).astype(BF16)
            total_out[c] = total
            sums[2 * c + sum_t] = total

            @pl.loop(0, n // 2)
            def _(k):
                target = 4 * far_first(k // 2, n // 4) + col * 2 + lax.rem(k, 2)

                @pl.when((target != me) & (target >= LEADS))
                def _():
                    give(total_out.at[c], target, 2 * c + sum_t)

    for c in range(heads):
        with jax.named_scope(f"w_back{c}"):
            for d in range(2):
                each(d, True, lambda d=d, c=c: back(d, c).wait_recv())
        for t in range(2):
            for i in range(nb):
                total = rback[0, c, i, t].astype(F32) + rback[1, c, i, t].astype(F32)
                own[c, i, t] = own[c, i, t] + total

    flag = jnp.where(owner_ref[0] == me, 1.0, 0.0)
    hot_out[...] = (jnp.concatenate([hot, hot], axis=1).astype(F32) * flag).astype(BF16)

    for c in range(heads):
        for d in range(2):
            for t in range(2):
                each(d, False, lambda d=d, c=c, t=t: halo(d, c, t).wait_send())
            each(d, False, lambda d=d, c=c: back(d, c).wait_send())

    @pl.when(odd)
    def _():
        for c in range(heads):
            pass_on(c).wait_send()

    @pl.when(mine_hub)
    def _():
        drain(hub_in, n // 2 - 1, hs_sem.at[1])

    @pl.when(adder)
    def _():
        for c in range(heads):
            drain(hub2_in.at[c], n // 2 - 1, hs_sem.at[3])
            cross(c).wait_send()

    @pl.when(adder & (col == 1))
    def _():
        drain(gpart, LEADS * heads, hs_sem.at[3])

    drain_own(gsend, heads, hs_sem.at[0], mine_hub)
    for self_served in range(2):
        @pl.when(adder if self_served else ~adder)
        def _():
            drain(gpart, heads * (2 - self_served), hs_sem.at[2])


    with jax.named_scope("w_gall2"):
        for who, count in ((lead, 4), (adder, 1), (~lead & ~adder, 2)):
            @pl.when(who)
            def _():
                drain(sums, count * heads, hr_sem.at[3])

    sums_out[...] = sums[...]


def write_out(heads, dq_ref, own, sums, hot, dq_out, dk_out, dv_out, dk_ref, dv_ref, sem):
    first = pltpu.make_async_copy(dq_ref, dq_out, sem.at[0])
    first.start()
    copies = [first]
    for t, (held, out) in enumerate(((dk_ref, dk_out), (dv_ref, dv_out))):
        for c in range(heads):
            both = jnp.concatenate([sums[2 * c + t], sums[2 * (heads + c) + t]], axis=0)
            extra = nn(hot[...], both)
            for i in range(own.shape[1]):
                rsl = slice(i * BLOCK, (i + 1) * BLOCK)
                held[0, rsl, c * DH : (c + 1) * DH] = (own[c, i, t] + extra[rsl]).astype(BF16)
        cp = pltpu.make_async_copy(held, out, sem.at[1 + t])
        cp.start()
        copies.append(cp)
    for cp in copies:
        cp.wait()


def solution(mesh):
    n = mesh.shape["seq"]

    def local(query, keys, values, grad_out, global_offset, owner, block_lists):
        rows, qw = query.shape[1:]
        kw = keys.shape[2]
        heads = kw // DH
        group = HQ // HK
        nb = rows // BLOCK
        listed = block_lists.shape[2]
        gtok = global_offset.shape[1]
        hubs = 2 * heads
        wide = nb + 2 * REACH
        assert nb == REACH and n % 8 == 0 and n >= 4 * hubs and heads == 2
        vm = pl.BlockSpec(memory_space=pltpu.VMEM)
        hb = pl.BlockSpec(memory_space=pl.ANY)
        held = pl.pallas_call(
            functools.partial(kernel, n, heads, group, nb, listed, gtok),
            out_shape=(
                pltpu.VMEM(query.shape, BF16),
                pltpu.VMEM((heads, nb, 2, BLOCK, DH), F32),
                pltpu.VMEM((4 * heads, gtok, DH), BF16),
                pltpu.VMEM((rows, 2 * gtok), BF16),
            ),
            in_specs=[hb] * 7,
            out_specs=(vm,) * 4,
            scratch_shapes=[
                pltpu.SMEM(owner.shape, jnp.int32),
                pltpu.SMEM(block_lists.shape, jnp.int32),
                pltpu.VMEM(global_offset.shape, jnp.int32),
                pltpu.SemaphoreType.DMA((3,)),
                pltpu.VMEM((rows, qw), BF16),
                pltpu.VMEM((rows, qw), BF16),
                pltpu.VMEM((2, heads, gtok, DH), BF16),
                pltpu.VMEM((n // 2, heads, gtok, DH), BF16),
                pltpu.VMEM((heads, gtok, DH), BF16),
                pltpu.SemaphoreType.DMA((heads,)),
                pltpu.VMEM((heads, 2, gtok, DH), BF16),
                pltpu.SemaphoreType.DMA((2 * heads,)),
                pltpu.VMEM((2 * heads, gtok, DH), BF16),
                pltpu.VMEM((heads, n // 2, gtok, DH), BF16),
                pltpu.VMEM((heads, gtok, DH), BF16),
                pltpu.VMEM((heads, gtok, DH), BF16),
                pltpu.VMEM((heads, gtok, DH), BF16),
                pltpu.VMEM((4 * heads, gtok, DH), BF16),
                pltpu.SemaphoreType.DMA((heads,)),
                pltpu.SemaphoreType.DMA((2 * heads,)),
                pltpu.VMEM((heads, nb, listed * BLOCK, group * BLOCK), F32),
                pltpu.VMEM((heads, nb, listed * BLOCK, group * BLOCK), F32),
                pltpu.VMEM((heads, nb, listed * BLOCK + gtok, group * BLOCK), BF16),
                pltpu.VMEM((nb, listed + 1, 2, BLOCK, DH), F32),
                pltpu.VMEM((2, heads, REACH, 2, BLOCK, DH), BF16),
                pltpu.VMEM((2, heads, REACH, 2, BLOCK, DH), BF16),
                pltpu.SemaphoreType.DMA((2 * heads * nb,)),
                pltpu.SemaphoreType.DMA((2,)),
                pltpu.SemaphoreType.DMA((4 * heads,)),
                pltpu.SemaphoreType.DMA((4 * heads,)),
                pltpu.SemaphoreType.DMA((2 * heads,)),
                pltpu.SemaphoreType.DMA((2 * heads,)),
                pltpu.SemaphoreType.DMA((4,)),
                pltpu.SemaphoreType.DMA((4,)),
            ]
            + [pltpu.VMEM((wide, BLOCK, DH), BF16)] * (2 * heads)
            + [pltpu.VMEM((4, gtok, DH), BF16)] * heads,
            compiler_params=pltpu.CompilerParams(collective_id=0, has_side_effects=True),
        )(owner, block_lists, global_offset, query, keys, values, grad_out)
        return pl.pallas_call(
            functools.partial(write_out, heads),
            out_shape=tuple(jax.ShapeDtypeStruct(a.shape, BF16) for a in (query, keys, values)),
            in_specs=[hb, vm, vm, vm],
            out_specs=[hb] * 3,
            scratch_shapes=[
                pltpu.VMEM(keys.shape, BF16),
                pltpu.VMEM(values.shape, BF16),
                pltpu.SemaphoreType.DMA((3,)),
            ],
        )(*[pltpu.with_memory_space_constraint(a, pltpu.VMEM) for a in held])

    return jax.shard_map(
        local,
        mesh=mesh,
        in_specs=(
            P(None, "seq", "head"),
            P(None, "seq", "head"),
            P(None, "seq", "head"),
            P(None, "seq", "head"),
            P(),
            P(),
            P(None, "seq", None),
        ),
        out_specs=(P(None, "seq", "head"), P(None, "seq", "head"), P(None, "seq", "head")),
        check_vma=False,
    )
```

```python
import functools

import jax
import jax.numpy as jnp
from jax import lax
from jax.experimental import pallas as pl
from jax.experimental.pallas import tpu as pltpu
from jax.sharding import PartitionSpec as P

HQ = 16
HK = 4
DH = 128
BLOCK = 128
REACH = 2
LEADS = 2
LOG2E = 1.4426950408889634
F32 = jnp.float32
BF16 = jnp.bfloat16


def nt(a, b):
    return lax.dot_general(a, b, (((1,), (1,)), ((), ())), preferred_element_type=F32)


def nn(a, b):
    return lax.dot_general(a, b, (((1,), (0,)), ((), ())), preferred_element_type=F32)


def kernel(
    n, heads, group, nb, listed, gtok,
    owner_hbm, lists_hbm, goff_hbm, q_hbm, k_hbm, v_hbm, g_hbm,
    dq_ref, own, sums_out, hot_out,
    owner_ref, lists_ref, goff_ref, small_sem, qv, gv, gsend, hub_in, hub_out, cand_sem, gall, fw_sem, gpart, hub2_in, half_out, total_out, cross_in, sums, sum_sem, cross_sem,
    keep_ex, keep_dp, keep_ds, wslot, sback, rback, load_sem, big_sem, ks_sem, kr_sem, gs_sem, gr_sem, hs_sem, hr_sem,
    *rest,
):
    kvw, gcand = rest[: 2 * heads], rest[2 * heads :]
    me = lax.axis_index("seq")
    hubs = 2 * heads
    rows = nb * BLOCK
    first = n // 2 - hubs + 1
    hub = (me - first) // 2
    col = lax.rem(me // 2, 2)
    lane = (me // 4) * 2 + lax.rem(me, 2)
    odd = lax.rem(me, 2) == 1
    level = hub // 2
    group_of = jnp.where(col == 0, level, heads - 1 - level)

    def row_of(g, side):
        return jnp.where(side == 0, g, heads - 1 - g)

    def hub_id(g, side):
        return first + 4 * row_of(g, side) + 2 * side

    def sum_id(t, side):
        return 4 * jnp.where(side == 0, 1 + t, 2 - t) + 2 * side + 1

    row = me // 4
    adder = odd & (row > 0) & (row < 3)
    sum_t = jnp.clip(jnp.where(col == 0, row - 1, 2 - row), 0, 1)
    other_sum = sum_id(sum_t, 1 - col)

    def hubbed(i):
        return (i >= first) & (i < first + 2 * hubs) & (lax.rem(i + first, 2) == 0)

    src_refs = (k_hbm, v_hbm)
    loads = []
    for t in range(2):
        for c in range(heads):
            for i in range(nb):
                cp = pltpu.make_async_copy(
                    src_refs[t].at[0, pl.ds(i * BLOCK, BLOCK), pl.ds(c * DH, DH)],
                    kvw[t * heads + c].at[REACH + i],
                    load_sem.at[(t * heads + c) * nb + i],
                )
                cp.start()
                loads.append(cp)
    small = [
        pltpu.make_async_copy(a, b, small_sem.at[i])
        for i, (a, b) in enumerate(
            ((goff_hbm, goff_ref), (owner_hbm, owner_ref), (lists_hbm, lists_ref))
        )
    ]
    for cp in small:
        cp.start()

    barrier = pltpu.get_barrier_semaphore()

    def greet(other):
        pl.semaphore_signal(
            barrier, inc=1, device_id={"seq": other}, device_id_type=pl.DeviceIdType.MESH
        )

    mine_hub = hubbed(me)

    @pl.when(mine_hub)
    def _():
        @pl.loop(0, n // 2)
        def _(k):
            target = (k // 2) * 4 + col * 2 + lax.rem(k, 2)

            @pl.when((target != me) & (target != me - 1))
            def _():
                greet(target)

    @pl.when(odd)
    def _():
        for g in range(heads):
            greet(hub_id(g, 1 - col))

    @pl.when(me > 0)
    def _():
        greet(me - 1)

    @pl.when(me < n - 1)
    def _():
        greet(me + 1)

    cq = pltpu.make_async_copy(q_hbm.at[0], qv, big_sem.at[0])
    cg = pltpu.make_async_copy(g_hbm.at[0], gv, big_sem.at[1])

    with jax.named_scope("w_loads"):
        small[0].wait()
        for cp in loads:
            cp.wait()
    cq.start()
    cg.start()

    hot = lax.broadcasted_iota(jnp.int32, (rows, gtok), 0) == goff_ref[...]
    hot = jnp.where(hot, 1.0, 0.0).astype(BF16)
    for t in range(2):
        for c in range(heads):
            mine = kvw[t * heads + c][REACH : REACH + nb].reshape(rows, DH)
            got = lax.dot_general(hot, mine, (((0,), (0,)), ((), ())), preferred_element_type=F32)
            gsend[t, c] = got.astype(BF16)
    zeros_kv = jnp.zeros((REACH, BLOCK, DH), BF16)

    @pl.when(me == 0)
    def _():
        for ref in kvw:
            ref[0:REACH] = zeros_kv
        rback[0] = jnp.zeros(rback.shape[1:], BF16)

    @pl.when(me == n - 1)
    def _():
        for ref in kvw:
            ref[REACH + nb : REACH + nb + REACH] = zeros_kv
        rback[1] = jnp.zeros(rback.shape[1:], BF16)

    lead = me < LEADS

    @pl.when(~lead)
    def _():
        sums[2 * heads :] = jnp.zeros((2 * heads, gtok, DH), BF16)

    zero_tile = jnp.zeros((nb, 2, BLOCK, DH), F32)
    wslot[:, listed] = zero_tile

    beside = jnp.where(me > 0, 1, 0) + jnp.where(me < n - 1, 1, 0)
    greeted = heads + jnp.where(mine_hub, n // 4 - 1, 0) - jnp.where(hubbed(me + 1), 1, 0)
    with jax.named_scope("w_barrier"):
        pl.semaphore_wait(barrier, beside + greeted)

    def remote(src, dst, s_sem, r_sem, target):
        return pltpu.make_async_remote_copy(
            src_ref=src, dst_ref=dst, send_sem=s_sem, recv_sem=r_sem,
            device_id={"seq": target}, device_id_type=pl.DeviceIdType.MESH,
        )

    def to_hub(src, dst, i, g, target):
        @pl.when(me != target)
        def _():
            remote(src.at[g], dst.at[lane], hs_sem.at[i], hr_sem.at[i], target).start()

    def drain(ref, count, sem):
        part = ref.at[pl.ds(0, count)]
        pltpu.make_async_copy(part, part, sem).wait()

    for g in range(heads):
        to_hub(gsend, hub_in, 0, g, hub_id(g, col))

    def halo(direction, c, t):
        idx = (direction * heads + c) * 2 + t
        ref = kvw[t * heads + c]
        if direction == 0:
            src, dst, target = ref.at[pl.ds(nb, REACH)], ref.at[pl.ds(0, REACH)], me + 1
        else:
            src, dst, target = ref.at[pl.ds(REACH, REACH)], ref.at[pl.ds(REACH + nb, REACH)], me - 1
        return remote(src, dst, ks_sem.at[idx], kr_sem.at[idx], target)

    def back(direction, c):
        idx = direction * heads + c
        target = me + 1 if direction == 0 else me - 1
        return remote(
            sback.at[direction, c], rback.at[direction, c], gs_sem.at[idx], gr_sem.at[idx], target
        )

    def each(direction, receiving, what):
        up = (direction == 0) != receiving
        cond = me < n - 1 if up else me > 0
        pl.when(cond)(what)

    place = lax.rem(me, 4)

    def far(d):
        return place == (3 if d == 0 else 0)

    def halo_start(c, d, late):
        for t in range(2):
            cond = (me < n - 1 if d == 0 else me > 0) & (far(d) if late else ~far(d))
            pl.when(cond)(lambda t=t: halo(d, c, t).start())

    held = mine_hub & (place == 1)

    halo_start(0, 0, False)
    halo_start(0, 1, False)
    for c in range(1, heads):
        halo_start(c, 1, False)
        pl.when(~held)(functools.partial(halo_start, c, 0, False))
    for c in range(heads):
        for d in range(2):
            halo_start(c, d, True)

    def halo_wait(c, paired):
        for d in range(2):
            cond = (me > 0 if d == 0 else me < n - 1) & ((odd if d == 0 else ~odd) == paired)
            for t in range(2):
                pl.when(cond)(lambda d=d, t=t: halo(d, c, t).wait_recv())

    for cp in small[1:]:
        cp.wait()

    with jax.named_scope('w_qg'):
        cq.wait()
        cg.wait()
    scale = DH ** (-0.5)
    fold = scale * LOG2E
    local_idx = [
        [
            jnp.clip(lists_ref[0, b, l] - me * nb + REACH, 0, nb + 2 * REACH - 1)
            for l in range(listed)
        ]
        for b in range(nb)
    ]

    def near_rows(t, c, b):
        return [kvw[t * heads + c][local_idx[b][l]] for l in range(1, listed)]

    def columns(c):
        return [slice((c * group + i) * DH, (c * group + i + 1) * DH) for i in range(group)]

    def stacked(ref, c, b):
        rsl = slice(b * BLOCK, (b + 1) * BLOCK)
        return jnp.concatenate([ref[rsl, s] for s in columns(c)], axis=0)

    def logits(ks, vs, c, b):
        return nt(ks, stacked(qv, c, b)), nt(vs, stacked(gv, c, b))

    def keep(c, b, start, st, dp):
        top = jnp.max(st, axis=0, keepdims=True)
        ex = jnp.exp2((st - top) * fold)
        keep_ex[c, b, start : start + st.shape[0]] = ex
        keep_dp[c, b, start : start + st.shape[0]] = dp
        total = jnp.sum(ex, axis=0, keepdims=True)
        return top, total, jnp.sum(ex * dp, axis=0, keepdims=True)

    window = listed * BLOCK
    stats = {}
    for c in range(heads):
        for b in range(nb):
            kb, vb = kvw[c][REACH + b], kvw[heads + c][REACH + b]
            stats[c, b] = [keep(c, b, 0, *logits(kb, vb, c, b))]

    def far_first(i, count):
        return jnp.where(lax.rem(i, 2) == 0, count - 1 - i // 2, i // 2)

    owner_at = owner_ref[0]

    @pl.when(mine_hub)
    def _():
        with jax.named_scope("w_hub1"):
            drain(hub_in, n // 2 - 1, hr_sem.at[0])
        hub_in[lane] = gsend[group_of]
        pick = hub_in[(owner_at // 4) * 2 + lax.rem(owner_at, 2)]
        hub_out[...] = pick
        for c in range(heads):
            gcand[c][2 * col + group_of] = pick[c]
        for c in range(heads):
            @pl.loop(0, n // 2)
            def _(k):
                target = 4 * far_first(k // 2, n // 4) + 2 * lax.rem(k, 2) + 1

                @pl.when(target != me)
                def _():
                    remote(
                        hub_out.at[c], gcand[c].at[2 * col + group_of],
                        hs_sem.at[1], cand_sem.at[c], target,
                    ).start()

        @pl.when(held)
        def _():
            for c in range(1, heads):
                halo_start(c, 0, False)

    held_back = adder & (place == 3) & (other_sum > me)

    def back_start(c):
        for d in range(2):
            if c == heads - 1 and d == 0:
                ready = (me < n - 1) & ~held_back
                pl.when(ready)(lambda d=d: back(d, c).start())
            else:
                each(d, False, lambda d=d: back(d, c).start())

    def drain_own(ref, count, sem, self_served):
        @pl.when(self_served)
        def _():
            drain(ref, count - 1, sem)

        @pl.when(~self_served)
        def _():
            drain(ref, count, sem)

    def pass_on(c):
        return remote(
            gall.at[c], gall.at[c], fw_sem.at[c], fw_sem.at[heads + c],
            jnp.where(odd, me - 1, me + 1),
        )

    def collect():
        side = lax.rem(owner_at // 2, 2) * 2
        for c in range(heads):
            with jax.named_scope(f"w_cand{c}"):
                drain_own(gcand[c], 4, cand_sem.at[c], mine_hub)
            for t in range(2):
                gall[c, t] = gcand[c][side + t]
            pass_on(c).start()

    ratios = {}

    def key_value_grads(c):
        for b in range(nb):
            qs, gs = stacked(qv, c, b), stacked(gv, c, b)
            own_ratio, near_ratio, dot = ratios[c, b]
            vals = []
            for lo, hi, ratio in ((0, BLOCK, own_ratio), (BLOCK, window, near_ratio)):
                pr = keep_ex[c, b, lo:hi] * ratio
                ds = (pr * (keep_dp[c, b, lo:hi] - dot)).astype(BF16)
                keep_ds[c, b, lo:hi] = ds
                vals.append((ds, pr.astype(BF16)))
            ds, pr = (jnp.concatenate([v[i] for v in vals], axis=0) for i in range(2))
            for t, val in enumerate((nn(ds, qs) * scale, nn(pr, gs))):
                for l in range(listed):
                    wslot[b, l, t] = val[l * BLOCK : (l + 1) * BLOCK]
        for dst in range(nb + 2 * REACH):
            total = None
            for b in range(nb):
                if not b <= dst <= b + 2 * REACH:
                    continue
                slot = jnp.int32(listed)
                for l in range(1, listed):
                    slot = jnp.where(local_idx[b][l] == dst, l, slot)
                term = wslot[b, 0] if dst == b + REACH else wslot[b, slot]
                total = term if total is None else total + term
            if dst < REACH:
                sback[1, c, dst] = total.astype(BF16)
            elif dst < REACH + nb:
                own[c, dst - REACH] = total
            else:
                sback[0, c, dst - REACH - nb] = total.astype(BF16)
        with jax.named_scope(f"s_back{c}"):
            back_start(c)

    for c in range(heads):
        last = c == heads - 1
        with jax.named_scope(f"w_halo{c}"):
            halo_wait(c, True)
            halo_wait(c, False)
        if not last:
            for b in range(nb):
                kn = jnp.concatenate(near_rows(0, c, b), axis=0)
                vn = jnp.concatenate(near_rows(1, c, b), axis=0)
                stats[c, b].append(keep(c, b, BLOCK, *logits(kn, vn, c, b)))
        if c == 0:
            pl.when(odd)(collect)
        with jax.named_scope(f"w_gall{c}"):
            @pl.when(~odd)
            def _():
                pass_on(c).wait_recv()
        glob = [None, None]
        for b in range(nb):
            qs, gs = stacked(qv, c, b), stacked(gv, c, b)
            kn, vn = [gall[c, 0]], [gall[c, 1]]
            if last:
                kn, vn = near_rows(0, c, b) + kn, near_rows(1, c, b) + vn
            st, dp = logits(jnp.concatenate(kn, axis=0), jnp.concatenate(vn, axis=0), c, b)
            top = jnp.max(st, axis=0, keepdims=True)
            for old in stats[c, b]:
                top = jnp.maximum(top, old[0])
            ex = jnp.exp2((st - top) * fold)
            total = jnp.sum(ex, axis=0, keepdims=True)
            dot = jnp.sum(ex * dp, axis=0, keepdims=True)
            shrinks = [jnp.exp2((old[0] - top) * fold) for old in stats[c, b]]
            for shrink, old in zip(shrinks, stats[c, b]):
                total = total + old[1] * shrink
                dot = dot + old[2] * shrink
            inv = 1.0 / total
            dot = dot * inv
            if last:
                near = window - BLOCK
                keep_ex[c, b, BLOCK:window] = ex[:near]
                keep_dp[c, b, BLOCK:window] = dp[:near]
                ex, dp = ex[near:], dp[near:]
            pr = ex * inv
            ds = (pr * (dp - dot)).astype(BF16)
            keep_ds[c, b, window:] = ds
            own_ratio = shrinks[0] * inv
            ratios[c, b] = (own_ratio, inv if last else shrinks[1] * inv, dot)
            for t, part in enumerate((nn(ds, qs) * scale, nn(pr.astype(BF16), gs))):
                glob[t] = part if glob[t] is None else glob[t] + part
        for t in range(2):
            gpart[2 * c + t] = glob[t].astype(BF16)
        with jax.named_scope(f"s_gpart{c}"):
            for t in range(2):
                target = sum_id(t, col)

                @pl.when(me != target)
                def _():
                    remote(
                        gpart.at[2 * c + t], hub2_in.at[c, lane], hs_sem.at[2], sum_sem.at[c], target
                    ).start()
        if c == 0:
            pl.when(odd)(functools.partial(key_value_grads, 0))

    pl.when(~odd)(functools.partial(key_value_grads, 0))
    for c in range(1, heads):
        key_value_grads(c)

    for c in range(heads):
        for b in range(nb):
            ks = jnp.concatenate([kvw[c][REACH + b]] + near_rows(0, c, b) + [gall[c, 0]], axis=0)
            dqt = nn(ks.T, keep_ds[c, b]) * scale
            dq = dqt.T.astype(BF16)
            for i, s in enumerate(columns(c)):
                dq_ref[0, b * BLOCK : (b + 1) * BLOCK, s] = dq[i * BLOCK : (i + 1) * BLOCK]

    def give(src, target, at):
        remote(src, sums.at[at], hs_sem.at[3], hr_sem.at[3], target).start()

    def cross(c):
        return remote(
            half_out.at[c], cross_in.at[c], cross_sem.at[c], cross_sem.at[heads + c], other_sum
        )

    @pl.when(adder)
    def _():
        halves = []
        for c in range(heads):
            with jax.named_scope(f"w_hub2{c}"):
                drain(hub2_in.at[c], n // 2 - 1, sum_sem.at[c])
            hub2_in[c, lane] = gpart[2 * c + sum_t]
            half = jnp.sum(hub2_in[c].astype(F32), axis=0)
            halves.append(half)
            half_out[c] = half.astype(BF16)
            cross(c).start()
            for target in range(LEADS):
                give(half_out.at[c], target, 2 * (col * heads + c) + sum_t)

        @pl.when(held_back)
        def _():
            back(0, heads - 1).start()

        for c in range(heads):
            with jax.named_scope(f"w_cross{c}"):
                cross(c).wait_recv()
            total = (halves[c] + cross_in[c].astype(F32)).astype(BF16)
            total_out[c] = total
            sums[2 * c + sum_t] = total

            @pl.loop(0, n // 2)
            def _(k):
                target = 4 * (k // 2) + col * 2 + lax.rem(k, 2)

                @pl.when((target != me) & (target >= LEADS))
                def _():
                    give(total_out.at[c], target, 2 * c + sum_t)

    for c in range(heads):
        with jax.named_scope(f"w_back{c}"):
            for d in range(2):
                each(d, True, lambda d=d, c=c: back(d, c).wait_recv())
        for t in range(2):
            for i in range(nb):
                total = rback[0, c, i, t].astype(F32) + rback[1, c, i, t].astype(F32)
                own[c, i, t] = own[c, i, t] + total

    flag = jnp.where(owner_ref[0] == me, 1.0, 0.0)
    hot_out[...] = (jnp.concatenate([hot, hot], axis=1).astype(F32) * flag).astype(BF16)

    for c in range(heads):
        for d in range(2):
            for t in range(2):
                each(d, False, lambda d=d, c=c, t=t: halo(d, c, t).wait_send())
            each(d, False, lambda d=d, c=c: back(d, c).wait_send())

    @pl.when(odd)
    def _():
        for c in range(heads):
            pass_on(c).wait_send()

    @pl.when(mine_hub)
    def _():
        drain(hub_in, n // 2 - 1, hs_sem.at[1])

    @pl.when(adder)
    def _():
        for c in range(heads):
            drain(hub2_in.at[c], n // 2 - 1, hs_sem.at[3])
            cross(c).wait_send()

    @pl.when(adder & (col == 1))
    def _():
        drain(gpart, LEADS * heads, hs_sem.at[3])

    drain_own(gsend, heads, hs_sem.at[0], mine_hub)
    for self_served in range(2):
        @pl.when(adder if self_served else ~adder)
        def _():
            drain(gpart, heads * (2 - self_served), hs_sem.at[2])


    with jax.named_scope("w_gall2"):
        for who, count in ((lead, 4), (adder, 1), (~lead & ~adder, 2)):
            @pl.when(who)
            def _():
                drain(sums, count * heads, hr_sem.at[3])

    sums_out[...] = sums[...]


def write_out(heads, dq_ref, own, sums, hot, dq_out, dk_out, dv_out, dk_ref, dv_ref, sem):
    first = pltpu.make_async_copy(dq_ref, dq_out, sem.at[0])
    first.start()
    copies = [first]
    for t, (held, out) in enumerate(((dk_ref, dk_out), (dv_ref, dv_out))):
        for c in range(heads):
            both = jnp.concatenate([sums[2 * c + t], sums[2 * (heads + c) + t]], axis=0)
            extra = nn(hot[...], both)
            for i in range(own.shape[1]):
                rsl = slice(i * BLOCK, (i + 1) * BLOCK)
                held[0, rsl, c * DH : (c + 1) * DH] = (own[c, i, t] + extra[rsl]).astype(BF16)
        cp = pltpu.make_async_copy(held, out, sem.at[1 + t])
        cp.start()
        copies.append(cp)
    for cp in copies:
        cp.wait()


def solution(mesh):
    n = mesh.shape["seq"]

    def local(query, keys, values, grad_out, global_offset, owner, block_lists):
        rows, qw = query.shape[1:]
        kw = keys.shape[2]
        heads = kw // DH
        group = HQ // HK
        nb = rows // BLOCK
        listed = block_lists.shape[2]
        gtok = global_offset.shape[1]
        hubs = 2 * heads
        wide = nb + 2 * REACH
        assert nb == REACH and n % 8 == 0 and n >= 4 * hubs and heads == 2
        vm = pl.BlockSpec(memory_space=pltpu.VMEM)
        hb = pl.BlockSpec(memory_space=pl.ANY)
        held = pl.pallas_call(
            functools.partial(kernel, n, heads, group, nb, listed, gtok),
            out_shape=(
                pltpu.VMEM(query.shape, BF16),
                pltpu.VMEM((heads, nb, 2, BLOCK, DH), F32),
                pltpu.VMEM((4 * heads, gtok, DH), BF16),
                pltpu.VMEM((rows, 2 * gtok), BF16),
            ),
            in_specs=[hb] * 7,
            out_specs=(vm,) * 4,
            scratch_shapes=[
                pltpu.SMEM(owner.shape, jnp.int32),
                pltpu.SMEM(block_lists.shape, jnp.int32),
                pltpu.VMEM(global_offset.shape, jnp.int32),
                pltpu.SemaphoreType.DMA((3,)),
                pltpu.VMEM((rows, qw), BF16),
                pltpu.VMEM((rows, qw), BF16),
                pltpu.VMEM((2, heads, gtok, DH), BF16),
                pltpu.VMEM((n // 2, heads, gtok, DH), BF16),
                pltpu.VMEM((heads, gtok, DH), BF16),
                pltpu.SemaphoreType.DMA((heads,)),
                pltpu.VMEM((heads, 2, gtok, DH), BF16),
                pltpu.SemaphoreType.DMA((2 * heads,)),
                pltpu.VMEM((2 * heads, gtok, DH), BF16),
                pltpu.VMEM((heads, n // 2, gtok, DH), BF16),
                pltpu.VMEM((heads, gtok, DH), BF16),
                pltpu.VMEM((heads, gtok, DH), BF16),
                pltpu.VMEM((heads, gtok, DH), BF16),
                pltpu.VMEM((4 * heads, gtok, DH), BF16),
                pltpu.SemaphoreType.DMA((heads,)),
                pltpu.SemaphoreType.DMA((2 * heads,)),
                pltpu.VMEM((heads, nb, listed * BLOCK, group * BLOCK), F32),
                pltpu.VMEM((heads, nb, listed * BLOCK, group * BLOCK), F32),
                pltpu.VMEM((heads, nb, listed * BLOCK + gtok, group * BLOCK), BF16),
                pltpu.VMEM((nb, listed + 1, 2, BLOCK, DH), F32),
                pltpu.VMEM((2, heads, REACH, 2, BLOCK, DH), BF16),
                pltpu.VMEM((2, heads, REACH, 2, BLOCK, DH), BF16),
                pltpu.SemaphoreType.DMA((2 * heads * nb,)),
                pltpu.SemaphoreType.DMA((2,)),
                pltpu.SemaphoreType.DMA((4 * heads,)),
                pltpu.SemaphoreType.DMA((4 * heads,)),
                pltpu.SemaphoreType.DMA((2 * heads,)),
                pltpu.SemaphoreType.DMA((2 * heads,)),
                pltpu.SemaphoreType.DMA((4,)),
                pltpu.SemaphoreType.DMA((4,)),
            ]
            + [pltpu.VMEM((wide, BLOCK, DH), BF16)] * (2 * heads)
            + [pltpu.VMEM((4, gtok, DH), BF16)] * heads,
            compiler_params=pltpu.CompilerParams(collective_id=0, has_side_effects=True),
        )(owner, block_lists, global_offset, query, keys, values, grad_out)
        return pl.pallas_call(
            functools.partial(write_out, heads),
            out_shape=tuple(jax.ShapeDtypeStruct(a.shape, BF16) for a in (query, keys, values)),
            in_specs=[hb, vm, vm, vm],
            out_specs=[hb] * 3,
            scratch_shapes=[
                pltpu.VMEM(keys.shape, BF16),
                pltpu.VMEM(values.shape, BF16),
                pltpu.SemaphoreType.DMA((3,)),
            ],
        )(*[pltpu.with_memory_space_constraint(a, pltpu.VMEM) for a in held])

    return jax.shard_map(
        local,
        mesh=mesh,
        in_specs=(
            P(None, "seq", "head"),
            P(None, "seq", "head"),
            P(None, "seq", "head"),
            P(None, "seq", "head"),
            P(),
            P(),
            P(None, "seq", None),
        ),
        out_specs=(P(None, "seq", "head"), P(None, "seq", "head"), P(None, "seq", "head")),
        check_vma=False,
    )
```
